32 devices in a mesh: gx: 4 (over z), gy: 8 (over y, x, core).
Axes of the slice: x: 2, y: 2, z: 4, core: 2. Of those that a mesh axis runs over, the one named last changes fastest.
Arguments:
- prolong: bfloat16 [2048, 24, 128], P(('gx', 'gy')), may hold values from -0.5 to 0.5
- stiffness: bfloat16 [4096, 4, 128, 128], P(('gx', 'gy')), may hold values from -6 to 6
- request: int32 [4096], P(('gx', 'gy')), may hold values from 0 to 63, as said below
- col_slot: int32 [4096, 4], P(('gx', 'gy')), may hold values from 0 to 127
- col_pos: int32 [4096, 4], P(('gx', 'gy')), may hold values from 0 to 15, as said below
- coarse_owner: int32 [2048, 1], P(('gx', 'gy')), may hold values from 0 to 31; in each aligned block of 64 rows (0 to 63, 64 to 127, ...) at most 4 rows name the same one
Outputs:
- coarse: float32 [4096, 24, 384], P(('gx', 'gy'))
The draws below stay inside these ranges and needn't reach their ends.
Inputs may be any that keep to these rules, and one draw needn't show every extreme that they name: `request`: on each device, entries k * 4 to (k + 1) * 4 - 1 name distinct aggregates of device k, as local indices there. `col_pos`: the 4 entries of one block row are distinct. `coarse_owner`: among one device's 64 aggregates at most 4 share a coarse owner, and on some devices 4 do.
All inputs are finite; a program needn't handle non-finite values.
Results may differ from the reference program's by a relative error of at most 0.0003.
Values may be sent and summed in bfloat16 or wider, within the bound.
A program may use at most 128 MiB of HBM per device.

```python
import math
import jax
import jax.numpy as jnp
import numpy as np
from jax import lax

AGG_DEV = 64
DOF = 128
CV = 24
MAXNB = 16
SLOT_DEV = 128
BPS = 4
SEND_MAX = 4
IN_ROWS = 128
NAGG = 2048
SLOTS = 4096
DEVICES = 32


def draw_request(key, part):
    per_peer = SLOT_DEV // DEVICES
    scores = jax.random.randint(key, (DEVICES * DEVICES, AGG_DEV), 0, 1 << 20) * AGG_DEV
    scores = scores + jnp.arange(AGG_DEV, dtype=jnp.int32)[None, :]
    chosen = jnp.argsort(scores, axis=1)[:, :per_peer]
    return chosen.reshape(-1).astype(jnp.int32)


def draw_col_pos(key, part):
    scores = jax.random.randint(key, (DEVICES * SLOT_DEV, MAXNB), 0, 1 << 20) * MAXNB
    scores = scores + jnp.arange(MAXNB, dtype=jnp.int32)[None, :]
    chosen = jnp.argsort(scores, axis=1)[:, :BPS]
    return chosen.astype(jnp.int32)


def touch_ends(values, key, low, high):
    longest = values.shape.index(max(values.shape))
    spots = []
    for shift in (0, 1):
        where = [jax.random.randint(jax.random.fold_in(key, axis), (), 0, length) for axis, length in enumerate(values.shape)]
        where[longest] = (where[longest] + shift) % values.shape[longest]
        spots.append(tuple(where))
    return values.at[spots[0]].set(low).at[spots[1]].set(high)


def level_of(own_key, shape, cuts, low, high):
    def one(position, shards_of):
        draws = jax.random.uniform(jax.random.fold_in(jax.random.fold_in(own_key, 6), position), (shards_of,), jnp.float32, low / len(cuts), high / len(cuts))
        return jnp.repeat(jnp.exp(draws), shape[position] // shards_of).reshape((-1,) + (1,) * (len(shape) - position - 1))

    factor_of = one(*cuts[0])
    for cut in cuts[1:]:
        factor_of = factor_of * one(*cut)
    return factor_of


def deal_out(stream_key, own, number, rows, count, top, reach, lean):
    order = jax.random.permutation(stream_key, count)
    heavy_load, common = load_shares(count, rows * top, reach, lean, True), load_shares(count, rows * top, reach, lean, False)
    places = jnp.arange(count)

    def named(sizes, offset_by):
        used = int((sizes > 0).sum())
        fixed = max(1, used // 4)
        shifted = fixed + (places - fixed + offset_by * (used - fixed)) % max(1, count - fixed)
        return jnp.zeros((count,), jnp.int32).at[order[jnp.where(places < fixed, places, shifted)]].set(jnp.asarray(sizes, jnp.int32))

    sizes = jnp.where(number % 4 == 0, named(heavy_load, number // 4), named(common, number - number // 4 - 1))
    mixed = jax.random.permutation(jax.random.fold_in(own, 3), count)
    source_of, taker = mixed[0:count // 2 * 2:2], mixed[1:count // 2 * 2:2]
    room = jnp.minimum(sizes[source_of] - 1, reach - sizes[taker]) // 2
    room = jnp.where((source_of == order[0]) | (taker == order[0]) | (sizes[taker] == 0), 0, jnp.maximum(room, 0))
    shifted = jax.random.randint(jax.random.fold_in(own, 4), (count // 2,), 0, 1 << 20) % (room + 1)
    sizes = sizes.at[source_of].add(-shifted).at[taker].add(shifted)
    items = jnp.searchsorted(jnp.cumsum(sizes), jnp.arange(rows * top), side="right").astype(jnp.int32)
    listing = items.reshape(top, rows).T
    listing = listing[jax.random.permutation(jax.random.fold_in(own, 1), rows)]
    offset_by = jax.random.randint(jax.random.fold_in(own, 2), (rows, 1), 0, top)
    return jnp.take_along_axis(listing, (jnp.arange(top)[None, :] + offset_by) % top, axis=1)


def load_shares(count, total, reach, slope, full):
    portions = [(1 << 20) // math.isqrt(rank ** slope) + 1 for rank in range(1, count + 1)]
    largest = reach if full else min(reach, max(-(-total // count), total * portions[0] // sum(portions)))
    least = 1 if total - largest >= count - 1 else 0
    holding, rest = [largest] + [least] * (count - 1), total - largest - least * (count - 1)
    while rest > 0:
        candidates = [i for i in range(1, count) if holding[i] < largest] or [i for i in range(1, count) if holding[i] < reach]
        whole, budget = sum([portions[i] for i in candidates]), rest
        for i in candidates:
            addition = min(reach - holding[i], max(1, budget * portions[i] // whole), rest)
            holding[i] = holding[i] + addition
            rest = rest - addition
    return np.array(holding)


def bell_draw(own_key, extent, width, limit, shards=(), held_as=jnp.bfloat16):
    values = width * jax.random.normal(own_key, extent, jnp.float32)
    if shards:
        values = values * level_of(own_key, extent, shards, -0.22, 0.18)
    return jnp.clip(values, -limit, limit).astype(held_as)


def setup_inputs(seed: int = 0) -> dict:
    arg_keys = jax.random.split(jax.random.key(seed), 7)
    prolong = bell_draw(arg_keys[0], (NAGG, CV, DOF), DOF ** -0.5, 0.5, ((0, 32),))
    stiffness = bell_draw(arg_keys[1], (SLOTS, BPS, DOF, DOF), 1.0, 6.0, ((0, 32),))
    request = draw_request(jax.random.fold_in(arg_keys[6], 71), 0)
    col_slot = touch_ends(jax.random.randint(arg_keys[3], (SLOTS, BPS), 0, SLOT_DEV), jax.random.fold_in(arg_keys[3], 1), 0, SLOT_DEV - 1).astype(jnp.int32)
    col_pos = draw_col_pos(jax.random.fold_in(arg_keys[6], 71), 0)
    coarse_owner_keys = jax.random.split(jax.random.fold_in(arg_keys[5], 1), NAGG // AGG_DEV)
    coarse_owner_turns = jax.random.permutation(jax.random.fold_in(arg_keys[5], 3), NAGG // AGG_DEV)
    coarse_owner = jax.vmap(lambda own, number: deal_out(jax.random.fold_in(arg_keys[5], 2), own, number, AGG_DEV, DEVICES, 1, SEND_MAX, 2))(coarse_owner_keys, coarse_owner_turns).reshape((NAGG, 1))
    return {"prolong": prolong, "stiffness": stiffness, "request": request, "col_slot": col_slot, "col_pos": col_pos, "coarse_owner": coarse_owner}


HIGH = lax.Precision.HIGHEST


def device_rows(prolong, stiff_block, request_block, slot_block, pos_block):
    per_peer = SLOT_DEV // DEVICES
    gid = (jnp.arange(SLOT_DEV, dtype=jnp.int32) // per_peer) * AGG_DEV + request_block.astype(jnp.int32)
    fetched = prolong[gid].astype(jnp.float32)
    col_rows = fetched[slot_block]
    applied = jnp.einsum("tqij,tqej->tqei", stiff_block.astype(jnp.float32), col_rows, precision=HIGH)
    partial_value = jnp.einsum("tci,tqei->tqce", fetched, applied, precision=HIGH)
    column_hot = (pos_block[:, :, None] == jnp.arange(MAXNB, dtype=jnp.int32)[None, None, :]).astype(jnp.float32)
    spread = jnp.einsum("tqce,tqn->tcne", partial_value, column_hot, precision=HIGH)
    return gid, spread.reshape(SLOT_DEV, CV, MAXNB * CV)


def reference(prolong, stiffness, request, col_slot, col_pos, coarse_owner):
    stiff_dev = stiffness.reshape(DEVICES, SLOT_DEV, BPS, DOF, DOF)
    request_dev = request.reshape(DEVICES, SLOT_DEV)
    slot_dev = col_slot.reshape(DEVICES, SLOT_DEV, BPS)
    pos_dev = col_pos.reshape(DEVICES, SLOT_DEV, BPS)

    def accumulate(total, pieces):
        gid, spread = device_rows(prolong, pieces[0], pieces[1], pieces[2], pieces[3])
        return total.at[gid].add(spread), None

    start = jnp.zeros((NAGG, CV, MAXNB * CV), jnp.float32)
    fine_coarse, _ = lax.scan(accumulate, start, (stiff_dev, request_dev, slot_dev, pos_dev))
    owners = coarse_owner[:, 0].reshape(DEVICES, AGG_DEV)
    peer_ids = jnp.arange(DEVICES, dtype=jnp.int32)
    owner_one = (owners[:, :, None] == peer_ids[None, None, :]).astype(jnp.int32)
    before = jnp.cumsum(owner_one, axis=1) - owner_one
    row_rank = jnp.sum(before * owner_one, axis=2)
    source = jnp.arange(DEVICES, dtype=jnp.int32)[:, None]
    target = (owners * IN_ROWS + source * SEND_MAX + row_rank).reshape(-1).astype(jnp.int32)
    coarse = jnp.zeros((DEVICES * IN_ROWS, CV, MAXNB * CV), jnp.float32).at[target].set(fine_coarse)
    return coarse
```

```python
import functools

import jax
import jax.numpy as jnp
from jax import lax
from jax.experimental import pallas as pl
from jax.experimental.pallas import tpu as pltpu
from jax.sharding import PartitionSpec as P

MAXNB = 16
AXES = ("gx", "gy")
LANES = 128
TOP = 32767.0
MESH = pl.DeviceIdType.MESH
HBM = pl.BlockSpec(memory_space=pl.ANY)
VMEM = pl.BlockSpec(memory_space=pltpu.VMEM)
SMEM = pl.BlockSpec(memory_space=pltpu.SMEM)
NT = (((1,), (1,)), ((), ()))


def peer_at(k, gx, gy, mixed):
    n = gx * gy
    x, y = lax.axis_index("gx"), lax.axis_index("gy")
    if gx % 2:
        return lax.rem(x * gy + y + 1 + k, n)
    half = gx // 2
    count = half * gy
    if mixed:
        near, i = lax.rem(k, 2), k // 2
    else:
        near, i = k // count, lax.rem(k, count)
    i = lax.rem(i + near, count)
    side = lax.rem(x // half + 1 + near, 2)
    row = side * half + lax.rem(x + i // gy, half)
    return row * gy + lax.rem(y + i, gy)


def deliver_kernel(dims, code_ref, scale_ref, out_ref, land_ref, land_scale, wide_ref, *sems):
    gx, gy, cv = dims
    code_send, code_recv, scale_send, scale_recv, out_sem = sems
    n, rows, width = code_ref.shape
    take = rows // cv
    me = lax.axis_index("gx") * gy + lax.axis_index("gy")
    barrier = pltpu.get_barrier_semaphore()

    def where(peer):
        return (peer // gy, lax.rem(peer, gy))

    def greet(k, c):
        peer = peer_at(k, gx, gy, True)
        pl.semaphore_signal(barrier, inc=1, device_id=where(peer), device_id_type=MESH)
        return c

    lax.fori_loop(0, n - 1, greet, 0)

    def copies(peer, source):
        return [
            pltpu.make_async_remote_copy(
                src_ref=src.at[peer], dst_ref=dst.at[source],
                send_sem=send.at[peer], recv_sem=recv.at[source],
                device_id=where(peer), device_id_type=MESH,
            )
            for src, dst, send, recv in (
                (scale_ref, land_scale, scale_send, scale_recv),
                (code_ref, land_ref, code_send, code_recv),
            )
        ]

    def out_copy(p):
        at = pl.ds(p * take, take)
        return pltpu.make_async_copy(wide_ref.at[at], out_ref.at[at], out_sem.at[p])

    pl.semaphore_wait(barrier, n - 1)

    def send(k, c):
        for copy in copies(peer_at(k, gx, gy, True), me):
            copy.start()
        return c

    lax.fori_loop(0, n - 1, send, 0)

    def decode(code, scale, p):
        values = code.astype(jnp.int32).astype(jnp.float32) * as_column(scale, rows)
        wide_ref[pl.ds(p * take, take)] = values.reshape(take, cv, width)
        out_copy(p).start()

    decode(code_ref[me], scale_ref[me], me)

    def drain(k, c):
        source = peer_at(k, gx, gy, True)
        for copy in copies(source, source):
            copy.wait()
        decode(land_ref[source], land_scale[source], source)
        return c

    lax.fori_loop(0, n - 1, drain, 0)

    def finish(p, c):
        out_copy(p).wait()
        return c

    lax.fori_loop(0, n, finish, 0)


def delivered(code, scale, cv, gx, gy):
    n, rows, width = code.shape
    sem = pltpu.SemaphoreType.DMA
    out = (n * rows // cv, cv, width)
    return pl.pallas_call(
        functools.partial(deliver_kernel, (gx, gy, cv)),
        out_shape=jax.ShapeDtypeStruct(out, jnp.float32),
        in_specs=[VMEM, VMEM],
        out_specs=HBM,
        scratch_shapes=[
            pltpu.VMEM(code.shape, jnp.int16),
            pltpu.VMEM(scale.shape, jnp.float32),
            pltpu.VMEM(out, jnp.float32),
        ]
        + [sem((n,))] * 5,
        compiler_params=pltpu.CompilerParams(
            collective_id=4, has_side_effects=True, vmem_limit_bytes=40 << 20
        ),
        name="delivered",
    )(code, scale)


def exchange_kernel(gx, gy, count, *refs):
    ins, outs = refs[:count], refs[count : 2 * count]
    send_sem, recv_sem, local_sem = refs[2 * count :]
    n = gx * gy
    me = lax.axis_index("gx") * gy + lax.axis_index("gy")
    barrier = pltpu.get_barrier_semaphore()

    def greet(k, c):
        peer = lax.rem(me + k, n)
        pl.semaphore_signal(barrier, inc=1, device_id=(peer // gy, lax.rem(peer, gy)), device_id_type=MESH)
        return c

    lax.fori_loop(1, n, greet, 0)
    own = [pltpu.make_async_copy(ins[i].at[me], outs[i].at[me], local_sem.at[i]) for i in range(count)]
    for copy in own:
        copy.start()
    pl.semaphore_wait(barrier, n - 1)

    def copies(k, source):
        peer = lax.rem(me + k, n)
        return [
            pltpu.make_async_remote_copy(
                src_ref=ins[i].at[peer],
                dst_ref=outs[i].at[source],
                send_sem=send_sem.at[i, k],
                recv_sem=recv_sem.at[i, k],
                device_id=(peer // gy, lax.rem(peer, gy)),
                device_id_type=MESH,
            )
            for i in range(count)
        ]

    def send(k, c):
        for copy in copies(k, me):
            copy.start()
        return c

    lax.fori_loop(1, n, send, 0)

    def drain(k, c):
        for copy in copies(k, lax.rem(me + n - k, n)):
            copy.wait()
        return c

    lax.fori_loop(1, n, drain, 0)
    for copy in own:
        copy.wait()


def exchange(arrays, gx, gy, number):
    count = len(arrays)
    n = gx * gy
    return pl.pallas_call(
        functools.partial(exchange_kernel, gx, gy, count),
        out_shape=[jax.ShapeDtypeStruct(a.shape, a.dtype) for a in arrays],
        in_specs=[HBM] * count,
        out_specs=[HBM] * count,
        scratch_shapes=[
            pltpu.SemaphoreType.DMA((count, n)),
            pltpu.SemaphoreType.DMA((count, n)),
            pltpu.SemaphoreType.DMA((count,)),
        ],
        compiler_params=pltpu.CompilerParams(collective_id=number, has_side_effects=True),
        name=f"exchange{number}",
    )(*arrays)


def as_row(column):
    rows = column.shape[0]
    shape = (rows, LANES)
    eye = lax.broadcasted_iota(jnp.int32, shape, 0) == lax.broadcasted_iota(jnp.int32, shape, 1)
    return jnp.sum(jnp.where(eye, column, 0.0), axis=0, keepdims=True)


def as_column(row, rows):
    shape = (rows, LANES)
    eye = lax.broadcasted_iota(jnp.int32, shape, 0) == lax.broadcasted_iota(jnp.int32, shape, 1)
    return jnp.sum(jnp.where(eye, row, 0.0), axis=1, keepdims=True)


def coded(values):
    top = jnp.maximum(jnp.max(jnp.abs(values), axis=1, keepdims=True), 1e-30)
    code = jnp.round(values * (TOP / top)).astype(jnp.int32).astype(jnp.int16)
    return code, as_row(top * (1.0 / TOP))


def group_product(dims, grp, slot_ref, wide_ref, cols_ref, mats_of):
    cv, bps, group = dims
    dof = wide_ref.shape[-1]
    span = bps * cv
    lane = lax.broadcasted_iota(jnp.int32, (dof, LANES), 1)
    applied = []
    for tl in range(group):
        for q in range(bps):
            block = wide_ref[slot_ref[grp * group + tl, q]]
            at = (span * tl + cv * q) % LANES
            first = min(cv, LANES - at)
            cols_ref[tl, at : at + first, :] = block[:first]
            if first < cv:
                cols_ref[tl, 0 : cv - first, :] = block[first:]
    for tl in range(group):
        cols = cols_ref[tl].astype(jnp.bfloat16)
        mats = mats_of(tl).reshape(bps * dof, dof)
        prod = lax.dot_general(mats, cols, NT, preferred_element_type=jnp.float32)
        rel = (lane + (LANES * tl - span * tl) % LANES) % LANES
        one = prod[(bps - 1) * dof :]
        for q in range(bps - 2, -1, -1):
            one = jnp.where(rel < cv * (q + 1), prod[q * dof : (q + 1) * dof], one)
        applied.append(one)
    tiles = []
    for j in range(span * group // LANES):
        low, high = LANES * j // span, (LANES * (j + 1) - 1) // span
        tile = applied[high]
        for tl in range(high - 1, low - 1, -1):
            tile = jnp.where(lane < span * (tl + 1) - LANES * j, applied[tl], tile)
        tiles.append(tile)
    whole = jnp.concatenate(tiles, axis=1)
    hi = whole.astype(jnp.bfloat16)
    lo = (whole - hi.astype(jnp.float32)).astype(jnp.bfloat16)
    rows = wide_ref[pl.ds(grp * group, group)].reshape(group * cv, dof).astype(jnp.bfloat16)
    both = jnp.dot(rows, hi, preferred_element_type=jnp.float32) + jnp.dot(
        rows, lo, preferred_element_type=jnp.float32
    )
    wide_lane = lax.broadcasted_iota(jnp.int32, (cv, span * group), 1)
    out = both[(group - 1) * cv :]
    for tl in range(group - 2, -1, -1):
        out = jnp.where(wide_lane < span * (tl + 1), both[tl * cv : (tl + 1) * cv], out)
    return out


def product_kernel(dims, slot_ref, fetched_ref, stiff_ref, out_ref, wide_ref, cols_ref):
    cv, bps, group, per_step = dims
    step = pl.program_id(0)

    @pl.when(step == 0)
    def _():
        wide_ref[...] = fetched_ref[...].astype(jnp.float32)

    def body(k, c):
        out_ref[k] = group_product(
            (cv, bps, group), step * per_step + k, slot_ref, wide_ref, cols_ref,
            lambda tl: stiff_ref[k * group + tl],
        )
        return c

    lax.fori_loop(0, per_step, body, 0)


def products(fetched, stiffness, col_slot, group):
    slots, cv, dof = fetched.shape
    bps = stiffness.shape[1]
    groups = slots // group
    per_step = 4 if groups % 4 == 0 else 1
    width = group * bps * cv
    return pl.pallas_call(
        functools.partial(product_kernel, (cv, bps, group, per_step)),
        grid=(groups // per_step,),
        out_shape=jax.ShapeDtypeStruct((groups, cv, width), jnp.float32),
        in_specs=[
            SMEM,
            pl.BlockSpec((slots, cv, dof), lambda i: (0, 0, 0)),
            pl.BlockSpec((per_step * group, bps, dof, dof), lambda i: (i, 0, 0, 0)),
        ],
        out_specs=pl.BlockSpec((per_step, cv, width), lambda i: (i, 0, 0)),
        scratch_shapes=[
            pltpu.VMEM((slots, cv, dof), jnp.float32),
            pltpu.VMEM((group, LANES, dof), jnp.float32),
        ],
        compiler_params=pltpu.CompilerParams(vmem_limit_bytes=48 << 20),
        name="products",
    )(col_slot, fetched, stiffness)


def offset_at(i, side, sign, gx, gy):
    half = gx // 2
    x, y = lax.axis_index("gx"), lax.axis_index("gy")
    row = lax.rem(lax.rem(x, half) + sign * (i // gy) + half, half)
    col = lax.rem(y + sign * lax.rem(i, gy) + gy, gy)
    return (side * half + row) * gy + col


def mixed_at(k, sign, gx, gy):
    count = gx // 2 * gy
    near = lax.rem(k, 2)
    side = lax.rem(lax.axis_index("gx") // (gx // 2) + 1 + near, 2)
    return offset_at(lax.rem(k // 2 + near, count), side, sign, gx, gy)


def group_tail(dims, grp, slot_ref, wide_ref, cols_ref, proj_ref):
    cv, bps, group = dims
    span = bps * cv
    lane = lax.broadcasted_iota(jnp.int32, (cv, LANES), 1)
    for tl in range(group):
        for q in range(bps):
            block = wide_ref[slot_ref[q, grp * group + tl]]
            at = (span * tl + cv * q) % LANES
            first = min(cv, LANES - at)
            cols_ref[tl, at : at + first, :] = block[:first]
            if first < cv:
                cols_ref[tl, 0 : cv - first, :] = block[first:]
    ends = []
    for tl in range(group):
        cols = cols_ref[tl].astype(jnp.bfloat16)
        prod = lax.dot_general(proj_ref[grp * group + tl], cols, NT, preferred_element_type=jnp.float32)
        both = prod[:span] + prod[span:]
        rel = (lane + (LANES * tl - span * tl) % LANES) % LANES
        one = both[(bps - 1) * cv :]
        for q in range(bps - 2, -1, -1):
            one = jnp.where(rel < cv * (q + 1), both[q * cv : (q + 1) * cv], one)
        ends.append(one)
    tiles = []
    for j in range(span * group // LANES):
        low, high = LANES * j // span, (LANES * (j + 1) - 1) // span
        tile = ends[high]
        for tl in range(high - 1, low - 1, -1):
            tile = jnp.where(lane < span * (tl + 1) - LANES * j, ends[tl], tile)
        tiles.append(tile)
    return jnp.concatenate(tiles, axis=1)


def fused_kernel(
    dims,
    slot_ref, meta_ref, prolong_ref, stiff_ref,
    meta_out, part_out, scale_out,
    meta_land, req_ref, stage_ref, fetched_ref, wide_ref, cols_ref, mats_ref, proj_ref, code_ref, factor_ref,
    meta_send, meta_recv, fetch_send, fetch_recv, part_send, part_recv, scale_send, scale_recv,
    mats_sem, own_sem,
):
    gx, gy, cv, bps, group = dims
    n = gx * gy
    count = n // 2
    span = bps * cv
    me = lax.axis_index("gx") * gy + lax.axis_index("gy")
    side = lax.axis_index("gx") // (gx // 2)
    barrier = pltpu.get_barrier_semaphore()

    def where(peer):
        return (peer // gy, lax.rem(peer, gy))

    def remote(src, dst, send_sem, recv_sem, peer):
        return pltpu.make_async_remote_copy(
            src_ref=src, dst_ref=dst, send_sem=send_sem, recv_sem=recv_sem,
            device_id=where(peer), device_id_type=MESH,
        )

    def meta_copy(peer, source):
        return remote(
            meta_ref.at[lax.rem(peer, count)], meta_land.at[source],
            meta_send.at[peer], meta_recv.at[source], peer,
        )

    def fetch_copy(peer, source):
        return remote(
            stage_ref.at[pl.ds(peer * group, group)],
            fetched_ref.at[pl.ds(source * group, group)],
            fetch_send.at[peer], fetch_recv.at[source], peer,
        )

    def part_copies(peer, source):
        at = lax.rem(peer, count)
        return (
            remote(factor_ref.at[at], scale_out.at[source], scale_send.at[peer], scale_recv.at[source], peer),
            remote(code_ref.at[at], part_out.at[source], part_send.at[peer], part_recv.at[source], peer),
        )

    def mats_copy(peer):
        return pltpu.make_async_copy(
            stiff_ref.at[pl.ds(peer * group, group)],
            mats_ref.at[pl.ds(peer * group, group)],
            mats_sem.at[peer],
        )

    def greet(k, c):
        pl.semaphore_signal(barrier, inc=1, device_id=where(lax.rem(me + k, n)), device_id_type=MESH)
        return c

    lax.fori_loop(1, n, greet, 0)
    own_meta = pltpu.make_async_copy(meta_ref.at[lax.rem(me, count)], meta_land.at[me], own_sem.at[0])
    own_meta.start()
    mats_copy(me).start()

    def load(k, c):
        mats_copy(mixed_at(k, -1, gx, gy)).start()
        return c

    lax.fori_loop(0, n - 1, load, 0)
    pl.semaphore_wait(barrier, n - 1)

    def ask(k, c):
        meta_copy(mixed_at(k, 1, gx, gy), me).start()
        return c

    lax.fori_loop(0, n - 1, ask, 0)
    own_meta.wait()

    def asked(k, c):
        source = mixed_at(k, -1, gx, gy)
        meta_copy(source, source).wait()
        return c

    lax.fori_loop(0, n - 1, asked, 0)
    to_scalars = pltpu.make_async_copy(meta_land, req_ref, own_sem.at[1])
    to_scalars.start()
    to_next = pltpu.make_async_copy(meta_land, meta_out, own_sem.at[2])
    to_next.start()
    to_scalars.wait()
    first = side * (group + group * bps)

    def fill(k, c):
        peer = mixed_at(k, 1, gx, gy)
        for j in range(group):
            stage_ref[peer * group + j] = prolong_ref[req_ref[peer, 0, first + j]]
        return c

    lax.fori_loop(0, n - 1, fill, 0)
    for j in range(group):
        stage_ref[me * group + j] = prolong_ref[req_ref[me, 0, first + j]]

    def answer(k, c):
        fetch_copy(mixed_at(k, 1, gx, gy), me).start()
        return c

    lax.fori_loop(0, n - 1, answer, 0)

    def project(source, from_ref):
        mats_copy(source).wait()
        for j in range(group):
            t = source * group + j
            block = from_ref[t]
            wide_ref[t] = block.astype(jnp.float32)
            mats = mats_ref[t]
            mats = jnp.concatenate([mats[q] for q in range(bps)], axis=1)
            prod = jnp.dot(block, mats, preferred_element_type=jnp.float32)
            rows = jnp.concatenate([prod[:, q * LANES : (q + 1) * LANES] for q in range(bps)], axis=0)
            hi = rows.astype(jnp.bfloat16)
            proj_ref[t, 0:span] = hi
            proj_ref[t, span : 2 * span] = (rows - hi.astype(jnp.float32)).astype(jnp.bfloat16)

    project(me, stage_ref)

    def take(k, c):
        source = mixed_at(k, -1, gx, gy)
        fetch_copy(source, source).wait_recv()
        project(source, fetched_ref)
        return c

    lax.fori_loop(0, n - 1, take, 0)

    def send(j, both):
        i = lax.rem(j + 1, count)
        for copy in part_copies(offset_at(i, 1 - side, 1, gx, gy), me):
            copy.start()
        if both:
            for copy in part_copies(offset_at(i, side, 1, gx, gy), me):
                copy.start()

    def work(j, c):
        at = lax.rem(offset_at(lax.rem(j + 1, count), side, 1, gx, gy), count)
        for u in range(2):
            out = group_tail(
                (cv, bps, group), u * count + at, slot_ref, wide_ref, cols_ref.at[u], proj_ref
            )
            code_ref[at, u], factor_ref[at, u] = coded(out)

        @pl.when(j > 0)
        def _():
            send(j - 1, True)

        return c

    lax.fori_loop(0, count, work, 0)
    send(count - 1, False)
    mine = lax.rem(me, count)
    own = (
        pltpu.make_async_copy(code_ref.at[mine], part_out.at[me], own_sem.at[3]),
        pltpu.make_async_copy(factor_ref.at[mine], scale_out.at[me], own_sem.at[4]),
    )
    for copy in own:
        copy.start()
    to_next.wait()

    def drain(k, c):
        source = mixed_at(k, -1, gx, gy)
        fetch_copy(source, source).wait_send()
        for copy in part_copies(source, source):
            copy.wait()
        return c

    lax.fori_loop(0, n - 1, drain, 0)
    for copy in own:
        copy.wait()


def fused(meta, prolong, stiffness, col_slot, gx, gy, group):
    slots, bps, dof, _ = stiffness.shape
    cv = prolong.shape[1]
    n = gx * gy
    count = n // 2
    width = group * bps * cv
    sem = pltpu.SemaphoreType.DMA
    return pl.pallas_call(
        functools.partial(fused_kernel, (gx, gy, cv, bps, group)),
        out_shape=[
            jax.ShapeDtypeStruct((n, 1, LANES), jnp.int32),
            jax.ShapeDtypeStruct((n, 2, cv, width), jnp.int16),
            jax.ShapeDtypeStruct((n, 2, 1, LANES), jnp.float32),
        ],
        in_specs=[SMEM, VMEM, VMEM, HBM],
        out_specs=[HBM, HBM, HBM],
        scratch_shapes=[
            pltpu.VMEM((n, 1, LANES), jnp.int32),
            pltpu.SMEM((n, 1, LANES), jnp.int32),
            pltpu.VMEM((slots, cv, dof), jnp.bfloat16),
            pltpu.VMEM((slots, cv, dof), jnp.bfloat16),
            pltpu.VMEM((slots, cv, dof), jnp.float32),
            pltpu.VMEM((2, group, LANES, dof), jnp.float32),
            pltpu.VMEM((slots, bps, dof, dof), jnp.bfloat16),
            pltpu.VMEM((slots, 2 * bps * cv, dof), jnp.bfloat16),
            pltpu.VMEM((count, 2, cv, width), jnp.int16),
            pltpu.VMEM((count, 2, 1, LANES), jnp.float32),
        ]
        + [sem((n,))] * 9
        + [sem((5,))],
        compiler_params=pltpu.CompilerParams(
            collective_id=1, has_side_effects=True, vmem_limit_bytes=40 << 20
        ),
        name="fused",
    )(col_slot, meta, prolong, stiffness)


def collect_kernel(dims, meta_ref, part_ref, scale_ref, total_ref, place_ref, seen_ref, item_ref, slot_ref):
    gx, gy, cv, bps, group, send_max, own_aggs, unroll = dims
    n = gx * gy
    count = n // 2
    span = bps * cv
    width = group * span
    trash = n * send_max
    me = lax.axis_index("gx") * gy + lax.axis_index("gy")
    side, mine = me // count, lax.rem(me, count)
    each = group + group * bps
    total_ref[...] = jnp.zeros_like(total_ref)

    def clear(i, c):
        seen_ref[i] = 0
        return c

    lax.fori_loop(0, 2 * n, clear, 0)

    def rank(a, c):
        for kk in range(2):
            owner = meta_ref[kk * count + mine, 0, 2 * each + a]
            before = seen_ref[kk * n + owner]
            seen_ref[kk * n + owner] = before + 1
            at = (lax.rem(owner, count) * 2 + kk) * send_max + before
            place_ref[kk * own_aggs + a] = jnp.where(owner // count == side, at, -1)
        return c

    lax.fori_loop(0, own_aggs, rank, 0, unroll=4)

    def listed(d, used):
        for kk in range(2):
            for tl in range(group):
                at = place_ref[kk * own_aggs + meta_ref[d, 0, kk * each + tl]]
                item_ref[used] = (d * 2 + kk) * group + tl
                slot_ref[used] = at
                used = used + jnp.where(at >= 0, 1, 0)
        return used

    used = lax.fori_loop(0, n, listed, 0, unroll=2)
    for u in range(unroll):
        item_ref[used + u] = 0
        slot_ref[used + u] = trash
    lane = lax.broadcasted_iota(jnp.int32, (cv, LANES), 1)
    ahead = lax.broadcasted_iota(jnp.int32, (cv, width), 1) - lax.broadcasted_iota(jnp.int32, (cv, width), 0)
    rest = jnp.zeros((LANES - span, width), jnp.float32)

    def body(g, c):
        for u in range(unroll):
            item = item_ref[g * unroll + u]
            slot = slot_ref[g * unroll + u]
            d, kk, tl = item // (2 * group), lax.rem(item // group, 2), lax.rem(item, group)
            begin = span * tl
            low, high = begin // LANES, (begin + span - 1) // LANES
            x0 = part_ref[d, kk, :, pl.ds(pl.multiple_of(low * LANES, LANES), LANES)].astype(jnp.int32)
            x1 = part_ref[d, kk, :, pl.ds(pl.multiple_of(high * LANES, LANES), LANES)].astype(jnp.int32)
            x = jnp.where(lane >= lax.rem(begin, LANES), x0, x1)
            x = pltpu.roll(x, lax.rem((LANES - span) * tl, LANES), 1)
            top = x >> 8
            stack = jnp.concatenate([top.astype(jnp.float32), (x - top * 256).astype(jnp.float32)], axis=0)
            hot = jnp.concatenate(
                [
                    jnp.where(ahead == cv * meta_ref[d, 0, kk * each + group + tl * bps + q], 1.0, 0.0)
                    for q in range(bps)
                ]
                + [rest],
                axis=0,
            )
            placed = jnp.dot(
                stack.astype(jnp.bfloat16), hot.astype(jnp.bfloat16), preferred_element_type=jnp.float32
            )
            rows = (placed[:cv] * 256.0 + placed[cv:]) * as_column(scale_ref[d, kk], cv)
            total_ref[slot] = total_ref[slot] + rows
        return c

    lax.fori_loop(0, (used + unroll - 1) // unroll, body, 0)


def collected(part, scale, meta, gx, gy, send_max, group, bps, own_aggs):
    n, _, cv, width = part.shape
    unroll = 4
    most = n * 2 * group + unroll
    return pl.pallas_call(
        functools.partial(collect_kernel, (gx, gy, cv, bps, group, send_max, own_aggs, unroll)),
        out_shape=jax.ShapeDtypeStruct((n * send_max + 1, cv, width), jnp.float32),
        in_specs=[SMEM, VMEM, VMEM],
        out_specs=VMEM,
        scratch_shapes=[
            pltpu.SMEM((2 * own_aggs,), jnp.int32),
            pltpu.SMEM((2 * n,), jnp.int32),
            pltpu.SMEM((most,), jnp.int32),
            pltpu.SMEM((most,), jnp.int32),
        ],
        compiler_params=pltpu.CompilerParams(vmem_limit_bytes=24 << 20),
        name="collected",
    )(meta, part, scale)


def handed_kernel(
    dims, total_ref, out_ref,
    code_ref, scale_ref, land_ref, land_scale, wide_ref,
    code_send, code_recv, scale_send, scale_recv, out_sem,
):
    gx, gy, send_max = dims
    n = gx * gy
    count = n // 2
    cv, width = total_ref.shape[1:]
    rows = send_max * cv
    me = lax.axis_index("gx") * gy + lax.axis_index("gy")
    side, mine = me // count, lax.rem(me, count)
    barrier = pltpu.get_barrier_semaphore()

    def where(at):
        peer = side * count + at
        return (peer // gy, lax.rem(peer, gy))

    def at_offset(i, sign):
        return lax.rem(offset_at(i, side, sign, gx, gy), count)

    def greet(k, c):
        pl.semaphore_signal(barrier, inc=1, device_id=where(at_offset(k, 1)), device_id_type=MESH)
        return c

    lax.fori_loop(1, count, greet, 0)

    def copies(peer, source):
        return [
            pltpu.make_async_remote_copy(
                src_ref=src.at[peer], dst_ref=dst.at[source],
                send_sem=send.at[peer], recv_sem=recv.at[source],
                device_id=where(peer), device_id_type=MESH,
            )
            for src, dst, send, recv in (
                (scale_ref, land_scale, scale_send, scale_recv),
                (code_ref, land_ref, code_send, code_recv),
            )
        ]

    def out_copy(p):
        at = pl.ds(p * send_max, send_max)
        return pltpu.make_async_copy(wide_ref.at[at], out_ref.at[at], out_sem.at[p])

    def own_copy(kk):
        return pltpu.make_async_copy(
            total_ref.at[pl.ds((mine * 2 + kk) * send_max, send_max)],
            out_ref.at[pl.ds((kk * count + mine) * send_max, send_max)],
            out_sem.at[kk * count + mine],
        )

    for kk in range(2):
        own_copy(kk).start()

    def code(i):
        at = at_offset(i, 1)
        for kk in range(2):
            values = total_ref[pl.ds((at * 2 + kk) * send_max, send_max)].reshape(rows, width)
            code_ref[at, kk], scale_ref[at, kk] = coded(values)

    def send(i):
        for copy in copies(at_offset(i, 1), mine):
            copy.start()

    code(1)
    pl.semaphore_wait(barrier, count - 1)

    def work(i, c):
        code(i)
        send(i - 1)
        return c

    lax.fori_loop(2, count, work, 0)
    send(count - 1)

    def drain(i, c):
        source = at_offset(i, -1)
        for copy in copies(source, source):
            copy.wait_recv()
        for kk in range(2):
            values = land_ref[source, kk].astype(jnp.int32).astype(jnp.float32)
            values = values * as_column(land_scale[source, kk], rows)
            p = kk * count + source
            wide_ref[pl.ds(p * send_max, send_max)] = values.reshape(send_max, cv, width)
            out_copy(p).start()
        return c

    lax.fori_loop(1, count, drain, 0)

    def finish(i, c):
        for copy in copies(at_offset(i, 1), mine):
            copy.wait_send()
        for kk in range(2):
            out_copy(kk * count + at_offset(i, 1)).wait()
        return c

    lax.fori_loop(1, count, finish, 0)
    for kk in range(2):
        own_copy(kk).wait()


def handed(total, send_max, gx, gy):
    n = gx * gy
    count = n // 2
    _, cv, width = total.shape
    sem = pltpu.SemaphoreType.DMA
    out = (n * send_max, cv, width)
    codes = (count, 2, send_max * cv, width)
    scales = (count, 2, 1, LANES)
    return pl.pallas_call(
        functools.partial(handed_kernel, (gx, gy, send_max)),
        out_shape=jax.ShapeDtypeStruct(out, jnp.float32),
        in_specs=[VMEM],
        out_specs=HBM,
        scratch_shapes=[
            pltpu.VMEM(codes, jnp.int16),
            pltpu.VMEM(scales, jnp.float32),
            pltpu.VMEM(codes, jnp.int16),
            pltpu.VMEM(scales, jnp.float32),
            pltpu.VMEM(out, jnp.float32),
        ]
        + [sem((count,))] * 4
        + [sem((n,))],
        compiler_params=pltpu.CompilerParams(
            collective_id=5, has_side_effects=True, vmem_limit_bytes=40 << 20
        ),
        name="handed",
    )(total)


def gather_rows_kernel(dims, meta_ref, owner_ref, part_ref, *refs):
    cv, bps, per_peer, group, send_max = dims
    out_ref, out_scale_ref, total_ref, place_ref, seen_ref = refs
    n = out_ref.shape[0]
    groups, _, width = part_ref.shape
    span = width // group
    total_ref[...] = jnp.zeros_like(total_ref)

    def clear(i, c):
        seen_ref[i] = 0
        return c

    lax.fori_loop(0, n, clear, 0)

    def rank(a, c):
        owner = owner_ref[a]
        before = seen_ref[owner]
        place_ref[a] = owner * send_max + before
        seen_ref[owner] = before + 1
        return c

    lax.fori_loop(0, owner_ref.shape[0], rank, 0)
    lane = lax.broadcasted_iota(jnp.int32, (cv, width), 1)
    column = lax.broadcasted_iota(jnp.int32, (width, width), 0)
    row_lane = lax.broadcasted_iota(jnp.int32, (1, width), 1)

    def body(g, c):
        at = row_lane
        for j in range(group * bps):
            t = g * group + j // bps
            pos = meta_ref[t // per_peer, 0, per_peer + (t % per_peer) * bps + j % bps]
            at = at + jnp.where(row_lane // cv == j, cv * (pos - j), 0)
        hot = jnp.where(column == at, 1.0, 0.0).astype(jnp.bfloat16)
        rest = part_ref[g]
        pieces = []
        for _ in range(3):
            piece = rest.astype(jnp.bfloat16).astype(jnp.float32)
            pieces.append(piece)
            rest = rest - piece
        placed = 0.0
        for piece in pieces:
            stack = jnp.concatenate(
                [
                    jnp.where((lane >= span * tl) & (lane < span * (tl + 1)), piece, 0.0)
                    for tl in range(group)
                ],
                axis=0,
            ).astype(jnp.bfloat16)
            placed = placed + lax.dot_general(
                stack, hot, NT, preferred_element_type=jnp.float32
            )
        for tl in range(group):
            t = g * group + tl
            where = place_ref[meta_ref[t // per_peer, 0, t % per_peer]]
            rows = placed[tl * cv : (tl + 1) * cv]
            total_ref[where] = total_ref[where] + rows
        return c

    lax.fori_loop(0, groups, body, 0, unroll=4)

    def emit(p, c):
        rows = total_ref[pl.ds(p * send_max, send_max)].reshape(send_max * cv, width)
        out_ref[p], out_scale_ref[p] = coded(rows)
        return c

    lax.fori_loop(0, n, emit, 0, unroll=4)


def gathered_rows(part, meta, owners, n, send_max, group, bps, per_peer):
    groups, cv, width = part.shape
    return pl.pallas_call(
        functools.partial(gather_rows_kernel, (cv, bps, per_peer, group, send_max)),
        out_shape=[
            jax.ShapeDtypeStruct((n, send_max * cv, width), jnp.int16),
            jax.ShapeDtypeStruct((n, 1, LANES), jnp.float32),
        ],
        in_specs=[SMEM, SMEM, VMEM],
        out_specs=[VMEM, VMEM],
        scratch_shapes=[
            pltpu.VMEM((n * send_max, cv, width), jnp.float32),
            pltpu.SMEM((owners.shape[0],), jnp.int32),
            pltpu.SMEM((n,), jnp.int32),
        ],
        compiler_params=pltpu.CompilerParams(vmem_limit_bytes=48 << 20),
        name="gathered_rows",
    )(meta, owners, part)


def per_device(gx, gy, prolong, stiffness, request, col_slot, col_pos, coarse_owner):
    n = gx * gy
    own_aggs, cv, dof = prolong.shape
    slots, bps = col_slot.shape
    per_peer = slots // n
    group = MAXNB // bps
    send_max = (2 * own_aggs + n - 1) // n
    each = per_peer + per_peer * bps
    halved = per_peer == group and gx % 2 == 0 and 2 * each + own_aggs <= LANES

    parts = jnp.concatenate([request.reshape(n, per_peer), col_pos.reshape(n, per_peer * bps)], axis=1)
    if halved:
        count = n // 2
        owners = jnp.broadcast_to(coarse_owner[:, 0], (count, own_aggs))
        meta = jnp.concatenate([parts[:count], parts[count:], owners], axis=1)
        meta = jnp.pad(meta, ((0, 0), (0, LANES - meta.shape[1])))[:, None, :]
        meta_in, part, scale = fused(meta, prolong, stiffness, col_slot.T, gx, gy, group)
        total = collected(part, scale, meta_in, gx, gy, send_max, group, bps, own_aggs)
        return handed(total, send_max, gx, gy)
    meta = jnp.pad(parts, ((0, 0), (0, LANES - each)))[:, None, :]
    (meta_in,) = exchange([meta], gx, gy, 1)
    answer = prolong[meta_in[:, 0, :per_peer].reshape(-1)].reshape(n, per_peer * cv, dof)
    (fetched,) = exchange([answer], gx, gy, 2)
    made = products(fetched.reshape(slots, cv, dof), stiffness, col_slot, group)
    flat = made.reshape(slots // group, cv, group, bps * cv).transpose(0, 2, 1, 3)
    (flat,) = exchange([flat.reshape(n, per_peer * cv, bps * cv)], gx, gy, 3)
    flat = flat.reshape(slots // group, group, cv, bps * cv).transpose(0, 2, 1, 3)
    part = flat.reshape(slots // group, cv, group * bps * cv)
    code, factor = gathered_rows(part, meta_in, coarse_owner[:, 0], n, send_max, group, bps, per_peer)
    return delivered(code, factor, cv, gx, gy)


def solution(mesh):
    gx, gy = mesh.shape["gx"], mesh.shape["gy"]
    placed = (
        P(AXES, None, None),
        P(AXES, None, None, None),
        P(AXES),
        P(AXES, None),
        P(AXES, None),
        P(AXES, None),
    )
    return jax.shard_map(
        functools.partial(per_device, gx, gy),
        mesh=mesh,
        in_specs=placed,
        out_specs=P(AXES, None, None),
        check_vma=False,
    )
```

```python
import functools

import jax
import jax.numpy as jnp
from jax import lax
from jax.experimental import pallas as pl
from jax.experimental.pallas import tpu as pltpu
from jax.sharding import PartitionSpec as P

MAXNB = 16
AXES = ("gx", "gy")
LANES = 128
TOP = 32767.0
ROWS = 8
MESH = pl.DeviceIdType.MESH
HBM = pl.BlockSpec(memory_space=pl.ANY)
VMEM = pl.BlockSpec(memory_space=pltpu.VMEM)
SMEM = pl.BlockSpec(memory_space=pltpu.SMEM)
NT = (((1,), (1,)), ((), ()))


def peer_at(k, gx, gy, mixed):
    n = gx * gy
    x, y = lax.axis_index("gx"), lax.axis_index("gy")
    if gx % 2:
        return lax.rem(x * gy + y + 1 + k, n)
    half = gx // 2
    count = half * gy
    if mixed:
        near, i = lax.rem(k, 2), k // 2
    else:
        near, i = k // count, lax.rem(k, count)
    i = lax.rem(i + near, count)
    side = lax.rem(x // half + 1 + near, 2)
    row = side * half + lax.rem(x + i // gy, half)
    return row * gy + lax.rem(y + i, gy)


def deliver_kernel(dims, code_ref, scale_ref, out_ref, land_ref, land_scale, wide_ref, *sems):
    gx, gy, cv = dims
    code_send, code_recv, scale_send, scale_recv, out_sem = sems
    n, rows, width = code_ref.shape
    take = rows // cv
    me = lax.axis_index("gx") * gy + lax.axis_index("gy")
    barrier = pltpu.get_barrier_semaphore()

    def where(peer):
        return (peer // gy, lax.rem(peer, gy))

    def greet(k, c):
        peer = peer_at(k, gx, gy, True)
        pl.semaphore_signal(barrier, inc=1, device_id=where(peer), device_id_type=MESH)
        return c

    lax.fori_loop(0, n - 1, greet, 0)

    def copies(peer, source):
        return [
            pltpu.make_async_remote_copy(
                src_ref=src.at[peer], dst_ref=dst.at[source],
                send_sem=send.at[peer], recv_sem=recv.at[source],
                device_id=where(peer), device_id_type=MESH,
            )
            for src, dst, send, recv in (
                (scale_ref, land_scale, scale_send, scale_recv),
                (code_ref, land_ref, code_send, code_recv),
            )
        ]

    def out_copy(p):
        at = pl.ds(p * take, take)
        return pltpu.make_async_copy(wide_ref.at[at], out_ref.at[at], out_sem.at[p])

    pl.semaphore_wait(barrier, n - 1)

    def send(k, c):
        for copy in copies(peer_at(k, gx, gy, True), me):
            copy.start()
        return c

    lax.fori_loop(0, n - 1, send, 0)

    def decode(code, scale, p):
        values = code.astype(jnp.int32).astype(jnp.float32) * as_column(scale, rows)
        wide_ref[pl.ds(p * take, take)] = values.reshape(take, cv, width)
        out_copy(p).start()

    decode(code_ref[me], scale_ref[me], me)

    def drain(k, c):
        source = peer_at(k, gx, gy, True)
        for copy in copies(source, source):
            copy.wait()
        decode(land_ref[source], land_scale[source], source)
        return c

    lax.fori_loop(0, n - 1, drain, 0)

    def finish(p, c):
        out_copy(p).wait()
        return c

    lax.fori_loop(0, n, finish, 0)


def delivered(code, scale, cv, gx, gy):
    n, rows, width = code.shape
    sem = pltpu.SemaphoreType.DMA
    out = (n * rows // cv, cv, width)
    return pl.pallas_call(
        functools.partial(deliver_kernel, (gx, gy, cv)),
        out_shape=jax.ShapeDtypeStruct(out, jnp.float32),
        in_specs=[VMEM, VMEM],
        out_specs=HBM,
        scratch_shapes=[
            pltpu.VMEM(code.shape, jnp.int16),
            pltpu.VMEM(scale.shape, jnp.float32),
            pltpu.VMEM(out, jnp.float32),
        ]
        + [sem((n,))] * 5,
        compiler_params=pltpu.CompilerParams(
            collective_id=4, has_side_effects=True, vmem_limit_bytes=40 << 20
        ),
        name="delivered",
    )(code, scale)


def exchange_kernel(gx, gy, count, *refs):
    ins, outs = refs[:count], refs[count : 2 * count]
    send_sem, recv_sem, local_sem = refs[2 * count :]
    n = gx * gy
    me = lax.axis_index("gx") * gy + lax.axis_index("gy")
    barrier = pltpu.get_barrier_semaphore()

    def greet(k, c):
        peer = lax.rem(me + k, n)
        pl.semaphore_signal(barrier, inc=1, device_id=(peer // gy, lax.rem(peer, gy)), device_id_type=MESH)
        return c

    lax.fori_loop(1, n, greet, 0)
    own = [pltpu.make_async_copy(ins[i].at[me], outs[i].at[me], local_sem.at[i]) for i in range(count)]
    for copy in own:
        copy.start()
    pl.semaphore_wait(barrier, n - 1)

    def copies(k, source):
        peer = lax.rem(me + k, n)
        return [
            pltpu.make_async_remote_copy(
                src_ref=ins[i].at[peer],
                dst_ref=outs[i].at[source],
                send_sem=send_sem.at[i, k],
                recv_sem=recv_sem.at[i, k],
                device_id=(peer // gy, lax.rem(peer, gy)),
                device_id_type=MESH,
            )
            for i in range(count)
        ]

    def send(k, c):
        for copy in copies(k, me):
            copy.start()
        return c

    lax.fori_loop(1, n, send, 0)

    def drain(k, c):
        for copy in copies(k, lax.rem(me + n - k, n)):
            copy.wait()
        return c

    lax.fori_loop(1, n, drain, 0)
    for copy in own:
        copy.wait()


def exchange(arrays, gx, gy, number):
    count = len(arrays)
    n = gx * gy
    return pl.pallas_call(
        functools.partial(exchange_kernel, gx, gy, count),
        out_shape=[jax.ShapeDtypeStruct(a.shape, a.dtype) for a in arrays],
        in_specs=[HBM] * count,
        out_specs=[HBM] * count,
        scratch_shapes=[
            pltpu.SemaphoreType.DMA((count, n)),
            pltpu.SemaphoreType.DMA((count, n)),
            pltpu.SemaphoreType.DMA((count,)),
        ],
        compiler_params=pltpu.CompilerParams(collective_id=number, has_side_effects=True),
        name=f"exchange{number}",
    )(*arrays)


def as_row(column):
    rows = column.shape[0]
    shape = (rows, LANES)
    eye = lax.broadcasted_iota(jnp.int32, shape, 0) == lax.broadcasted_iota(jnp.int32, shape, 1)
    return jnp.sum(jnp.where(eye, column, 0.0), axis=0, keepdims=True)


def as_column(row, rows, first=0):
    shape = (rows, LANES)
    eye = lax.broadcasted_iota(jnp.int32, shape, 0) + first == lax.broadcasted_iota(jnp.int32, shape, 1)
    return jnp.sum(jnp.where(eye, row, 0.0), axis=1, keepdims=True)


def coded(values):
    top = jnp.maximum(jnp.max(jnp.abs(values), axis=1, keepdims=True), 1e-30)
    code = jnp.round(values * (TOP / top)).astype(jnp.int32).astype(jnp.int16)
    return code, as_row(top * (1.0 / TOP))


def group_product(dims, grp, slot_ref, wide_ref, cols_ref, mats_of):
    cv, bps, group = dims
    dof = wide_ref.shape[-1]
    span = bps * cv
    lane = lax.broadcasted_iota(jnp.int32, (dof, LANES), 1)
    applied = []
    for tl in range(group):
        for q in range(bps):
            block = wide_ref[slot_ref[grp * group + tl, q]]
            at = (span * tl + cv * q) % LANES
            first = min(cv, LANES - at)
            cols_ref[tl, at : at + first, :] = block[:first]
            if first < cv:
                cols_ref[tl, 0 : cv - first, :] = block[first:]
    for tl in range(group):
        cols = cols_ref[tl].astype(jnp.bfloat16)
        mats = mats_of(tl).reshape(bps * dof, dof)
        prod = lax.dot_general(mats, cols, NT, preferred_element_type=jnp.float32)
        rel = (lane + (LANES * tl - span * tl) % LANES) % LANES
        one = prod[(bps - 1) * dof :]
        for q in range(bps - 2, -1, -1):
            one = jnp.where(rel < cv * (q + 1), prod[q * dof : (q + 1) * dof], one)
        applied.append(one)
    tiles = []
    for j in range(span * group // LANES):
        low, high = LANES * j // span, (LANES * (j + 1) - 1) // span
        tile = applied[high]
        for tl in range(high - 1, low - 1, -1):
            tile = jnp.where(lane < span * (tl + 1) - LANES * j, applied[tl], tile)
        tiles.append(tile)
    whole = jnp.concatenate(tiles, axis=1)
    hi = whole.astype(jnp.bfloat16)
    lo = (whole - hi.astype(jnp.float32)).astype(jnp.bfloat16)
    rows = wide_ref[pl.ds(grp * group, group)].reshape(group * cv, dof).astype(jnp.bfloat16)
    both = jnp.dot(rows, hi, preferred_element_type=jnp.float32) + jnp.dot(
        rows, lo, preferred_element_type=jnp.float32
    )
    wide_lane = lax.broadcasted_iota(jnp.int32, (cv, span * group), 1)
    out = both[(group - 1) * cv :]
    for tl in range(group - 2, -1, -1):
        out = jnp.where(wide_lane < span * (tl + 1), both[tl * cv : (tl + 1) * cv], out)
    return out


def product_kernel(dims, slot_ref, fetched_ref, stiff_ref, out_ref, wide_ref, cols_ref):
    cv, bps, group, per_step = dims
    step = pl.program_id(0)

    @pl.when(step == 0)
    def _():
        wide_ref[...] = fetched_ref[...].astype(jnp.float32)

    def body(k, c):
        out_ref[k] = group_product(
            (cv, bps, group), step * per_step + k, slot_ref, wide_ref, cols_ref,
            lambda tl: stiff_ref[k * group + tl],
        )
        return c

    lax.fori_loop(0, per_step, body, 0)


def products(fetched, stiffness, col_slot, group):
    slots, cv, dof = fetched.shape
    bps = stiffness.shape[1]
    groups = slots // group
    per_step = 4 if groups % 4 == 0 else 1
    width = group * bps * cv
    return pl.pallas_call(
        functools.partial(product_kernel, (cv, bps, group, per_step)),
        grid=(groups // per_step,),
        out_shape=jax.ShapeDtypeStruct((groups, cv, width), jnp.float32),
        in_specs=[
            SMEM,
            pl.BlockSpec((slots, cv, dof), lambda i: (0, 0, 0)),
            pl.BlockSpec((per_step * group, bps, dof, dof), lambda i: (i, 0, 0, 0)),
        ],
        out_specs=pl.BlockSpec((per_step, cv, width), lambda i: (i, 0, 0)),
        scratch_shapes=[
            pltpu.VMEM((slots, cv, dof), jnp.float32),
            pltpu.VMEM((group, LANES, dof), jnp.float32),
        ],
        compiler_params=pltpu.CompilerParams(vmem_limit_bytes=48 << 20),
        name="products",
    )(col_slot, fetched, stiffness)


def offset_at(i, side, sign, gx, gy):
    half = gx // 2
    x, y = lax.axis_index("gx"), lax.axis_index("gy")
    row = lax.rem(lax.rem(x, half) + sign * (i // gy) + half, half)
    col = lax.rem(y + sign * lax.rem(i, gy) + gy, gy)
    return (side * half + row) * gy + col


def mixed_at(k, sign, gx, gy):
    count = gx // 2 * gy
    near = lax.rem(k, 2)
    side = lax.rem(lax.axis_index("gx") // (gx // 2) + 1 + near, 2)
    return offset_at(lax.rem(k // 2 + near, count), side, sign, gx, gy)


def arrival_at(k, gx, gy):
    count = gx // 2 * gy
    near = lax.rem(k, 2)
    side = lax.rem(lax.axis_index("gx") // (gx // 2) + 1 + near, 2)
    return offset_at(lax.rem(k // 2 + 1, count), side, -1, gx, gy)


def slot_matrix(dims, meta_land, meta_flat, side, mine):
    n, count, bps, group, send_max = dims
    each = group + group * bps
    square = (LANES, LANES)
    sub = lax.broadcasted_iota(jnp.int32, square, 0)
    lane = lax.broadcasted_iota(jnp.int32, square, 1)
    for d in range(n):
        meta_flat[d : d + 1] = meta_land[d]
    flat = meta_flat[...].astype(jnp.float32).astype(jnp.bfloat16)
    places = []
    for kk in range(2):
        owner = meta_land[kk * count + mine]
        value = owner.astype(jnp.float32)
        same = (as_column(value, LANES) == value) & (sub < lane) & (sub >= 2 * each)
        rank = jnp.sum(jnp.where(same, 1.0, 0.0), axis=0, keepdims=True)
        at = ((lax.rem(owner, count) * 2 + kk) * send_max).astype(jnp.float32) + rank
        places.append(as_column(jnp.where(owner // count == side, at, -1.0), LANES))
    second = lax.rem(lane // group, 2)
    source = lax.broadcasted_iota(jnp.int32, (n, LANES), 0)
    taken = lax.broadcasted_iota(jnp.int32, (n, LANES), 1) // (2 * group)
    pick = jnp.where(sub == second * each + lax.rem(lane, group), 1.0, 0.0).astype(jnp.bfloat16)
    every = jnp.dot(flat, pick, preferred_element_type=jnp.float32)
    place = jnp.where(second == 0, places[0], places[1])
    pieces = []
    for half in range(2 * n * group // LANES):
        first = half * (LANES // (2 * group))
        asked = jnp.sum(jnp.where(source == taken + first, every, 0.0), axis=0, keepdims=True)
        hit = sub.astype(jnp.float32) == asked + 2.0 * each
        slot = jnp.sum(jnp.where(hit, place, 0.0), axis=0, keepdims=True)
        pieces.append(jnp.where(sub.astype(jnp.float32) == slot, 1.0, 0.0))
    return jnp.concatenate(pieces, axis=1).astype(jnp.bfloat16)


def group_tail(dims, grp, slot_ref, wide_ref, cols_ref, proj_ref):
    cv, bps, group = dims
    span = bps * cv
    lane = lax.broadcasted_iota(jnp.int32, (cv, LANES), 1)
    for tl in range(group):
        for q in range(bps):
            block = wide_ref[slot_ref[q, grp * group + tl]]
            at = (span * tl + cv * q) % LANES
            first = min(cv, LANES - at)
            cols_ref[tl, at : at + first, :] = block[:first]
            if first < cv:
                cols_ref[tl, 0 : cv - first, :] = block[first:]
    ends = []
    for tl in range(group):
        cols = cols_ref[tl].astype(jnp.bfloat16)
        prod = lax.dot_general(proj_ref[grp * group + tl], cols, NT, preferred_element_type=jnp.float32)
        both = prod[:span] + prod[span:]
        rel = (lane + (LANES * tl - span * tl) % LANES) % LANES
        one = both[(bps - 1) * cv :]
        for q in range(bps - 2, -1, -1):
            one = jnp.where(rel < cv * (q + 1), both[q * cv : (q + 1) * cv], one)
        ends.append(one)
    tiles = []
    for j in range(span * group // LANES):
        low, high = LANES * j // span, (LANES * (j + 1) - 1) // span
        tile = ends[high]
        for tl in range(high - 1, low - 1, -1):
            tile = jnp.where(lane < span * (tl + 1) - LANES * j, ends[tl], tile)
        tiles.append(tile)
    return jnp.concatenate(tiles, axis=1)


def meta_row(dims, r, asked_row, pos_rows, owner_row):
    count, bps, group = dims
    each = group + group * bps
    lane = lax.broadcasted_iota(jnp.int32, (1, LANES), 1)
    row = owner_row[...]
    for kk in range(2):
        for tl in range(group):
            t = (kk * count + r) * group + tl
            row = jnp.where(lane == kk * each + tl, asked_row[0, t], row)
            for q in range(bps):
                row = jnp.where(lane == kk * each + group + tl * bps + q, pos_rows[q, t], row)
    return row


def fused_kernel(
    dims,
    asked_ref, pos_ref, owner_ref, slot_in, prolong_in, stiff_ref,
    out_ref,
    asked_row, pos_rows, owner_row, slot_ref, prolong_ref, meta_ref,
    meta_land, meta_flat, req_ref, stage_ref, fetched_ref, wide_ref, cols_ref, mats_ref, proj_ref,
    code_ref, factor_ref, part_ref, scale_ref, select_ref, placed_ref, total_ref,
    sent_ref, sent_scale, land_ref, land_scale, final_ref,
    meta_send, meta_recv, fetch_send, fetch_recv, part_send, part_recv, scale_send, scale_recv,
    row_send, row_recv, unit_send, unit_recv, out_sem, mats_sem, own_sem,
):
    gx, gy, cv, bps, group, send_max = dims
    n = gx * gy
    count = n // 2
    span = bps * cv
    width = group * span
    each = group + group * bps
    steps = cv // ROWS
    slots = 2 * send_max
    me = lax.axis_index("gx") * gy + lax.axis_index("gy")
    side, mine = me // count, lax.rem(me, count)
    barrier = pltpu.get_barrier_semaphore()

    def where(peer):
        return (peer // gy, lax.rem(peer, gy))

    def remote(src, dst, send_sem, recv_sem, peer):
        return pltpu.make_async_remote_copy(
            src_ref=src, dst_ref=dst, send_sem=send_sem, recv_sem=recv_sem,
            device_id=where(peer), device_id_type=MESH,
        )

    def meta_copy(peer, source):
        return remote(
            meta_ref.at[lax.rem(peer, count)], meta_land.at[source],
            meta_send.at[peer], meta_recv.at[source], peer,
        )

    def fetch_copy(peer, source):
        return remote(
            stage_ref.at[pl.ds(peer * group, group)],
            fetched_ref.at[pl.ds(source * group, group)],
            fetch_send.at[peer], fetch_recv.at[source], peer,
        )

    def part_copy(h, peer, source):
        return remote(
            code_ref.at[lax.rem(peer, count), h], part_ref.at[source, h],
            part_send.at[h, peer], part_recv.at[h, source], peer,
        )

    def scale_copy(peer, source):
        return remote(
            factor_ref.at[lax.rem(peer, count)], scale_ref.at[source],
            scale_send.at[peer], scale_recv.at[source], peer,
        )

    def row_copies(h, peer, source):
        device = side * count + peer
        return (
            remote(
                sent_scale.at[h, peer], land_scale.at[h, source],
                unit_send.at[h, peer], unit_recv.at[h, source], device,
            ),
            remote(
                sent_ref.at[h, peer], land_ref.at[h, source],
                row_send.at[h, peer], row_recv.at[h, source], device,
            ),
        )

    def out_copies(source):
        return [
            pltpu.make_async_copy(
                final_ref.at[source, pl.ds(kk * send_max, send_max)],
                out_ref.at[pl.ds((kk * count + source) * send_max, send_max)],
                out_sem.at[kk * count + source],
            )
            for kk in range(2)
        ]

    def by_turn(i, sign):
        i = lax.rem(i, 2) * (count // 2) + i // 2
        return lax.rem(offset_at(i, side, sign, gx, gy), count)

    def mats_copy(peer):
        return pltpu.make_async_copy(
            stiff_ref.at[pl.ds(peer * group, group)],
            mats_ref.at[pl.ds(peer * group, group)],
            mats_sem.at[peer],
        )

    def greet(k, c):
        pl.semaphore_signal(barrier, inc=1, device_id=where(lax.rem(me + k, n)), device_id_type=MESH)
        return c

    small = [
        pltpu.make_async_copy(src, dst, own_sem.at[2 + i])
        for i, (src, dst) in enumerate((
            (asked_ref, asked_row), (pos_ref, pos_rows), (owner_ref, owner_row),
            (prolong_in, prolong_ref), (slot_in, slot_ref),
        ))
    ]
    for copy in small:
        copy.start()
    lax.fori_loop(1, n, greet, 0)
    for copy in small[:3]:
        copy.wait()

    def note(r, c):
        meta_ref[r] = meta_row((count, bps, group), r, asked_row, pos_rows, owner_row)
        return c

    lax.fori_loop(0, count, note, 0, unroll=2)
    own_meta = pltpu.make_async_copy(meta_ref.at[lax.rem(me, count)], meta_land.at[me], own_sem.at[0])
    mats_copy(me).start()

    def load(k, c):
        mats_copy(mixed_at(k, -1, gx, gy)).start()
        return c

    lax.fori_loop(0, n - 1, load, 0)
    own_meta.start()
    pl.semaphore_wait(barrier, n - 1)

    def ask(k, c):
        meta_copy(mixed_at(k, 1, gx, gy), me).start()
        return c

    lax.fori_loop(0, n - 1, ask, 0)
    own_meta.wait()

    def asked(k, c):
        source = mixed_at(k, -1, gx, gy)
        meta_copy(source, source).wait()
        return c

    lax.fori_loop(0, n - 1, asked, 0)
    to_scalars = pltpu.make_async_copy(meta_land, req_ref, own_sem.at[1])
    to_scalars.start()
    small[3].wait()
    small[4].wait()
    to_scalars.wait()
    first = side * each

    def fill(k, c):
        peer = mixed_at(k, 1, gx, gy)
        for j in range(group):
            stage_ref[peer * group + j] = prolong_ref[req_ref[peer, 0, first + j]]
        return c

    lax.fori_loop(0, n - 1, fill, 0)
    for j in range(group):
        stage_ref[me * group + j] = prolong_ref[req_ref[me, 0, first + j]]

    def answer(k, c):
        fetch_copy(mixed_at(k, 1, gx, gy), me).start()
        return c

    lax.fori_loop(0, n - 1, answer, 0)

    def project(source, from_ref):
        mats_copy(source).wait()
        for j in range(group):
            t = source * group + j
            block = from_ref[t]
            wide_ref[t] = block.astype(jnp.float32)
            mats = mats_ref[t]
            mats = jnp.concatenate([mats[q] for q in range(bps)], axis=1)
            prod = jnp.dot(block, mats, preferred_element_type=jnp.float32)
            rows = jnp.concatenate([prod[:, q * LANES : (q + 1) * LANES] for q in range(bps)], axis=0)
            hi = rows.astype(jnp.bfloat16)
            proj_ref[t, 0:span] = hi
            proj_ref[t, span : 2 * span] = (rows - hi.astype(jnp.float32)).astype(jnp.bfloat16)

    select_ref[...] = slot_matrix((n, count, bps, group, send_max), meta_land, meta_flat, side, mine)
    project(me, stage_ref)

    def take(k, c):
        source = mixed_at(k, -1, gx, gy)
        fetch_copy(source, source).wait_recv()
        project(source, fetched_ref)
        return c

    lax.fori_loop(0, n - 1, take, 0)

    def send(h, j, both):
        i = lax.rem(j + 1, count)
        far = offset_at(i, 1 - side, 1, gx, gy)
        near = offset_at(i, side, 1, gx, gy)
        for peer in (far, near) if both else (far,):
            if h == 0:
                scale_copy(peer, me).start()
            part_copy(h, peer, me).start()

    def work(j, c):
        at = lax.rem(offset_at(lax.rem(j + 1, count), side, 1, gx, gy), count)
        for u in range(2):
            out = group_tail(
                (cv, bps, group), u * count + at, slot_ref, wide_ref, cols_ref.at[u], proj_ref
            )
            top = jnp.maximum(jnp.max(jnp.abs(out), axis=1, keepdims=True), 1e-30)
            code = jnp.round(out * (TOP / top)).astype(jnp.int32)
            for h in range(steps):
                code_ref[at, h, u] = code[h * ROWS : (h + 1) * ROWS].astype(jnp.int16)
            factor_ref[at, u] = as_row(top * (1.0 / TOP))

        @pl.when(j > 0)
        def _():
            send(0, j - 1, True)

        return c

    lax.fori_loop(0, count, work, 0)
    send(0, count - 1, False)
    for h in range(1, steps):

        def more(j, c):
            send(h, j, True)
            return c

        lax.fori_loop(0, count - 1, more, 0)
        send(h, count - 1, False)

    lane = lax.broadcasted_iota(jnp.int32, (ROWS, LANES), 1)
    column = [(lane + LANES * j) // cv for j in range(width // LANES)]

    def place(h, d, from_ref, from_scale, at):
        blocks = []
        for kk in range(2):
            v = from_ref[at, h, kk].astype(jnp.int32).astype(jnp.float32)
            v = v * as_column(from_scale[at, kk], ROWS, h * ROWS)
            for tl in range(group):
                begin = span * tl
                low, high = begin // LANES * LANES, (begin + span - 1) // LANES * LANES
                x = v[:, low : low + LANES]
                if high > low:
                    x = jnp.where(lane >= begin % LANES, x, v[:, high : high + LANES])
                tiles = [jnp.zeros((ROWS, LANES), jnp.float32) for _ in column]
                for q in range(bps):
                    pos = req_ref[d, 0, kk * each + group + tl * bps + q]
                    moved = pltpu.roll(x, lax.rem(cv * pos + 8 * LANES - begin - cv * q, LANES), 1)
                    tiles = [jnp.where(col == pos, moved, tile) for col, tile in zip(column, tiles)]
                blocks.append(jnp.concatenate(tiles, axis=1))
        rows = pl.ds(pl.multiple_of(d * ROWS, ROWS), ROWS)
        placed_ref[:, rows, :] = jnp.swapaxes(jnp.stack(blocks), 0, 1)

    def decode(h, source, from_ref, from_scale):
        values = from_ref[h, source].astype(jnp.int32).astype(jnp.float32)
        values = values * as_column(from_scale[h, source], slots * ROWS)
        final_ref[source, :, h * ROWS : (h + 1) * ROWS, :] = values.reshape(slots, ROWS, width)
        if h == steps - 1:
            for copy in out_copies(source):
                copy.start()

    def decode_all(h):
        decode(h, mine, sent_ref, sent_scale)

        def one(i, c):
            source = by_turn(i, -1)
            for copy in row_copies(h, source, source):
                copy.wait_recv()
            decode(h, source, land_ref, land_scale)
            return c

        lax.fori_loop(1, count, one, 0)

    for h in range(steps):
        place(h, me, code_ref, factor_ref, mine)

        def arrive(k, c):
            source = arrival_at(k, gx, gy)
            if h == 0:
                scale_copy(source, source).wait_recv()
            part_copy(h, source, source).wait_recv()
            place(h, source, part_ref, scale_ref, source)
            return c

        lax.fori_loop(0, n - 1, arrive, 0)

        def gather(r, c):
            x = placed_ref[r]
            hi = x.astype(jnp.bfloat16)
            lo = (x - hi.astype(jnp.float32)).astype(jnp.bfloat16)
            select = select_ref[...]
            got = jnp.dot(select, hi, preferred_element_type=jnp.float32)
            got = got + jnp.dot(select, lo, preferred_element_type=jnp.float32)
            total_ref[r] = got
            return c

        lax.fori_loop(0, ROWS, gather, 0)

        def pack(i):
            peer = by_turn(i, 1)
            values = total_ref[:, pl.ds(pl.multiple_of(peer * slots, slots), slots), :]
            values = jnp.swapaxes(values, 0, 1).reshape(slots * ROWS, width)
            sent_ref[h, peer], sent_scale[h, peer] = coded(values)

        def hand(i):
            for copy in row_copies(h, by_turn(i, 1), mine):
                copy.start()

        pack(1)

        def pass_on(i, c):
            pack(i)
            hand(i - 1)
            return c

        lax.fori_loop(2, count, pass_on, 0)
        pack(0)
        hand(count - 1)
        if h > 0:
            decode_all(h - 1)
    decode_all(steps - 1)

    def drain(k, c):
        peer = mixed_at(k, 1, gx, gy)
        fetch_copy(peer, me).wait_send()
        scale_copy(peer, me).wait_send()
        for h in range(steps):
            part_copy(h, peer, me).wait_send()
        return c

    lax.fori_loop(0, n - 1, drain, 0)

    def finish(i, c):
        for h in range(steps):
            for copy in row_copies(h, by_turn(i, 1), mine):
                copy.wait_send()
        return c

    lax.fori_loop(1, count, finish, 0)

    def written(i, c):
        for copy in out_copies(i):
            copy.wait()
        return c

    lax.fori_loop(0, count, written, 0)


def fused(asked, pos, owners, slots_of, prolong, stiffness, gx, gy, group, send_max):
    slots, bps, dof, _ = stiffness.shape
    cv = prolong.shape[1]
    n = gx * gy
    count = n // 2
    width = group * bps * cv
    steps = cv // ROWS
    taken = 2 * n * group
    rows = 2 * send_max * ROWS
    sem = pltpu.SemaphoreType.DMA
    return pl.pallas_call(
        functools.partial(fused_kernel, (gx, gy, cv, bps, group, send_max)),
        out_shape=jax.ShapeDtypeStruct((n * send_max, cv, width), jnp.float32),
        in_specs=[HBM] * 6,
        out_specs=HBM,
        scratch_shapes=[
            pltpu.SMEM(asked.shape, jnp.int32),
            pltpu.SMEM(pos.shape, jnp.int32),
            pltpu.VMEM(owners.shape, jnp.int32),
            pltpu.SMEM(slots_of.shape, jnp.int32),
            pltpu.VMEM(prolong.shape, jnp.bfloat16),
            pltpu.VMEM((count, 1, LANES), jnp.int32),
            pltpu.VMEM((n, 1, LANES), jnp.int32),
            pltpu.VMEM((n, LANES), jnp.int32),
            pltpu.SMEM((n, 1, LANES), jnp.int32),
            pltpu.VMEM((slots, cv, dof), jnp.bfloat16),
            pltpu.VMEM((slots, cv, dof), jnp.bfloat16),
            pltpu.VMEM((slots, cv, dof), jnp.float32),
            pltpu.VMEM((2, group, LANES, dof), jnp.float32),
            pltpu.VMEM((slots, bps, dof, dof), jnp.bfloat16),
            pltpu.VMEM((slots, 2 * bps * cv, dof), jnp.bfloat16),
            pltpu.VMEM((count, steps, 2, ROWS, width), jnp.int16),
            pltpu.VMEM((count, 2, 1, LANES), jnp.float32),
            pltpu.VMEM((n, steps, 2, ROWS, width), jnp.int16),
            pltpu.VMEM((n, 2, 1, LANES), jnp.float32),
            pltpu.VMEM((n * send_max, taken), jnp.bfloat16),
            pltpu.VMEM((ROWS, taken, width), jnp.float32),
            pltpu.VMEM((ROWS, n * send_max, width), jnp.float32),
            pltpu.VMEM((steps, count, rows, width), jnp.int16),
            pltpu.VMEM((steps, count, 1, LANES), jnp.float32),
            pltpu.VMEM((steps, count, rows, width), jnp.int16),
            pltpu.VMEM((steps, count, 1, LANES), jnp.float32),
            pltpu.VMEM((count, 2 * send_max, cv, width), jnp.float32),
        ]
        + [sem((n,))] * 4
        + [sem((steps, n))] * 2
        + [sem((n,))] * 2
        + [sem((steps, count))] * 4
        + [sem((n,))] * 2
        + [sem((7,))],
        compiler_params=pltpu.CompilerParams(
            collective_id=1, has_side_effects=True, vmem_limit_bytes=54 << 20
        ),
        name="fused",
    )(asked, pos, owners, slots_of, prolong, stiffness)


def gather_rows_kernel(dims, meta_ref, owner_ref, part_ref, *refs):
    cv, bps, per_peer, group, send_max = dims
    out_ref, out_scale_ref, total_ref, place_ref, seen_ref = refs
    n = out_ref.shape[0]
    groups, _, width = part_ref.shape
    span = width // group
    total_ref[...] = jnp.zeros_like(total_ref)

    def clear(i, c):
        seen_ref[i] = 0
        return c

    lax.fori_loop(0, n, clear, 0)

    def rank(a, c):
        owner = owner_ref[a]
        before = seen_ref[owner]
        place_ref[a] = owner * send_max + before
        seen_ref[owner] = before + 1
        return c

    lax.fori_loop(0, owner_ref.shape[0], rank, 0)
    lane = lax.broadcasted_iota(jnp.int32, (cv, width), 1)
    column = lax.broadcasted_iota(jnp.int32, (width, width), 0)
    row_lane = lax.broadcasted_iota(jnp.int32, (1, width), 1)

    def body(g, c):
        at = row_lane
        for j in range(group * bps):
            t = g * group + j // bps
            pos = meta_ref[t // per_peer, 0, per_peer + (t % per_peer) * bps + j % bps]
            at = at + jnp.where(row_lane // cv == j, cv * (pos - j), 0)
        hot = jnp.where(column == at, 1.0, 0.0).astype(jnp.bfloat16)
        rest = part_ref[g]
        pieces = []
        for _ in range(3):
            piece = rest.astype(jnp.bfloat16).astype(jnp.float32)
            pieces.append(piece)
            rest = rest - piece
        placed = 0.0
        for piece in pieces:
            stack = jnp.concatenate(
                [
                    jnp.where((lane >= span * tl) & (lane < span * (tl + 1)), piece, 0.0)
                    for tl in range(group)
                ],
                axis=0,
            ).astype(jnp.bfloat16)
            placed = placed + lax.dot_general(
                stack, hot, NT, preferred_element_type=jnp.float32
            )
        for tl in range(group):
            t = g * group + tl
            where = place_ref[meta_ref[t // per_peer, 0, t % per_peer]]
            rows = placed[tl * cv : (tl + 1) * cv]
            total_ref[where] = total_ref[where] + rows
        return c

    lax.fori_loop(0, groups, body, 0, unroll=4)

    def emit(p, c):
        rows = total_ref[pl.ds(p * send_max, send_max)].reshape(send_max * cv, width)
        out_ref[p], out_scale_ref[p] = coded(rows)
        return c

    lax.fori_loop(0, n, emit, 0, unroll=4)


def gathered_rows(part, meta, owners, n, send_max, group, bps, per_peer):
    groups, cv, width = part.shape
    return pl.pallas_call(
        functools.partial(gather_rows_kernel, (cv, bps, per_peer, group, send_max)),
        out_shape=[
            jax.ShapeDtypeStruct((n, send_max * cv, width), jnp.int16),
            jax.ShapeDtypeStruct((n, 1, LANES), jnp.float32),
        ],
        in_specs=[SMEM, SMEM, VMEM],
        out_specs=[VMEM, VMEM],
        scratch_shapes=[
            pltpu.VMEM((n * send_max, cv, width), jnp.float32),
            pltpu.SMEM((owners.shape[0],), jnp.int32),
            pltpu.SMEM((n,), jnp.int32),
        ],
        compiler_params=pltpu.CompilerParams(vmem_limit_bytes=48 << 20),
        name="gathered_rows",
    )(meta, owners, part)


def per_device(gx, gy, prolong, stiffness, request, col_slot, col_pos, coarse_owner):
    n = gx * gy
    own_aggs, cv, dof = prolong.shape
    slots, bps = col_slot.shape
    per_peer = slots // n
    group = MAXNB // bps
    send_max = (2 * own_aggs + n - 1) // n
    each = per_peer + per_peer * bps
    halved = per_peer == group and gx % 2 == 0 and slots == LANES and cv % ROWS == 0 and 2 * group == ROWS == 2 * send_max and 2 * each + own_aggs <= LANES

    if halved:
        owners = jnp.pad(coarse_owner.T, ((0, 0), (2 * each, LANES - own_aggs - 2 * each)))
        held = (request[None], col_pos.T, owners, col_slot.T, prolong, stiffness)
        held = [pltpu.with_memory_space_constraint(a, pltpu.HBM) for a in held]
        return fused(*held, gx, gy, group, send_max)
    meta = jnp.concatenate([request.reshape(n, per_peer), col_pos.reshape(n, per_peer * bps)], axis=1)
    meta = jnp.pad(meta, ((0, 0), (0, LANES - each)))[:, None, :]
    (meta_in,) = exchange([meta], gx, gy, 1)
    answer = prolong[meta_in[:, 0, :per_peer].reshape(-1)].reshape(n, per_peer * cv, dof)
    (fetched,) = exchange([answer], gx, gy, 2)
    made = products(fetched.reshape(slots, cv, dof), stiffness, col_slot, group)
    flat = made.reshape(slots // group, cv, group, bps * cv).transpose(0, 2, 1, 3)
    (flat,) = exchange([flat.reshape(n, per_peer * cv, bps * cv)], gx, gy, 3)
    flat = flat.reshape(slots // group, group, cv, bps * cv).transpose(0, 2, 1, 3)
    part = flat.reshape(slots // group, cv, group * bps * cv)
    code, factor = gathered_rows(part, meta_in, coarse_owner[:, 0], n, send_max, group, bps, per_peer)
    return delivered(code, factor, cv, gx, gy)


def solution(mesh):
    gx, gy = mesh.shape["gx"], mesh.shape["gy"]
    placed = (
        P(AXES, None, None),
        P(AXES, None, None, None),
        P(AXES),
        P(AXES, None),
        P(AXES, None),
        P(AXES, None),
    )
    return jax.shard_map(
        functools.partial(per_device, gx, gy),
        mesh=mesh,
        in_specs=placed,
        out_specs=P(AXES, None, None),
        check_vma=False,
    )
```

```python
import functools

import jax
import jax.numpy as jnp
from jax import lax
from jax.experimental import pallas as pl
from jax.experimental.pallas import tpu as pltpu
from jax.sharding import PartitionSpec as P

MAXNB = 16
AXES = ("gx", "gy")
LANES = 128
TOP = 32767.0
ROWS = 8
PAIR = 1
DEEP = 1
MESH = pl.DeviceIdType.MESH
HBM = pl.BlockSpec(memory_space=pl.ANY)
VMEM = pl.BlockSpec(memory_space=pltpu.VMEM)
SMEM = pl.BlockSpec(memory_space=pltpu.SMEM)
NT = (((1,), (1,)), ((), ()))


def peer_at(k, gx, gy, mixed):
    n = gx * gy
    x, y = lax.axis_index("gx"), lax.axis_index("gy")
    if gx % 2:
        return lax.rem(x * gy + y + 1 + k, n)
    half = gx // 2
    count = half * gy
    if mixed:
        near, i = lax.rem(k, 2), k // 2
    else:
        near, i = k // count, lax.rem(k, count)
    i = lax.rem(i + near, count)
    side = lax.rem(x // half + 1 + near, 2)
    row = side * half + lax.rem(x + i // gy, half)
    return row * gy + lax.rem(y + i, gy)


def deliver_kernel(dims, code_ref, scale_ref, out_ref, land_ref, land_scale, wide_ref, *sems):
    gx, gy, cv = dims
    code_send, code_recv, scale_send, scale_recv, out_sem = sems
    n, rows, width = code_ref.shape
    take = rows // cv
    me = lax.axis_index("gx") * gy + lax.axis_index("gy")
    barrier = pltpu.get_barrier_semaphore()

    def where(peer):
        return (peer // gy, lax.rem(peer, gy))

    def greet(k, c):
        peer = peer_at(k, gx, gy, True)
        pl.semaphore_signal(barrier, inc=1, device_id=where(peer), device_id_type=MESH)
        return c

    lax.fori_loop(0, n - 1, greet, 0)

    def copies(peer, source):
        return [
            pltpu.make_async_remote_copy(
                src_ref=src.at[peer], dst_ref=dst.at[source],
                send_sem=send.at[peer], recv_sem=recv.at[source],
                device_id=where(peer), device_id_type=MESH,
            )
            for src, dst, send, recv in (
                (scale_ref, land_scale, scale_send, scale_recv),
                (code_ref, land_ref, code_send, code_recv),
            )
        ]

    def out_copy(p):
        at = pl.ds(p * take, take)
        return pltpu.make_async_copy(wide_ref.at[at], out_ref.at[at], out_sem.at[p])

    pl.semaphore_wait(barrier, n - 1)

    def send(k, c):
        for copy in copies(peer_at(k, gx, gy, True), me):
            copy.start()
        return c

    lax.fori_loop(0, n - 1, send, 0)

    def decode(code, scale, p):
        values = code.astype(jnp.int32).astype(jnp.float32) * as_column(scale, rows)
        wide_ref[pl.ds(p * take, take)] = values.reshape(take, cv, width)
        out_copy(p).start()

    decode(code_ref[me], scale_ref[me], me)

    def drain(k, c):
        source = peer_at(k, gx, gy, True)
        for copy in copies(source, source):
            copy.wait()
        decode(land_ref[source], land_scale[source], source)
        return c

    lax.fori_loop(0, n - 1, drain, 0)

    def finish(p, c):
        out_copy(p).wait()
        return c

    lax.fori_loop(0, n, finish, 0)


def delivered(code, scale, cv, gx, gy):
    n, rows, width = code.shape
    sem = pltpu.SemaphoreType.DMA
    out = (n * rows // cv, cv, width)
    return pl.pallas_call(
        functools.partial(deliver_kernel, (gx, gy, cv)),
        out_shape=jax.ShapeDtypeStruct(out, jnp.float32),
        in_specs=[VMEM, VMEM],
        out_specs=HBM,
        scratch_shapes=[
            pltpu.VMEM(code.shape, jnp.int16),
            pltpu.VMEM(scale.shape, jnp.float32),
            pltpu.VMEM(out, jnp.float32),
        ]
        + [sem((n,))] * 5,
        compiler_params=pltpu.CompilerParams(
            collective_id=4, has_side_effects=True, vmem_limit_bytes=40 << 20
        ),
        name="delivered",
    )(code, scale)


def exchange_kernel(gx, gy, count, *refs):
    ins, outs = refs[:count], refs[count : 2 * count]
    send_sem, recv_sem, local_sem = refs[2 * count :]
    n = gx * gy
    me = lax.axis_index("gx") * gy + lax.axis_index("gy")
    barrier = pltpu.get_barrier_semaphore()

    def greet(k, c):
        peer = lax.rem(me + k, n)
        pl.semaphore_signal(barrier, inc=1, device_id=(peer // gy, lax.rem(peer, gy)), device_id_type=MESH)
        return c

    lax.fori_loop(1, n, greet, 0)
    own = [pltpu.make_async_copy(ins[i].at[me], outs[i].at[me], local_sem.at[i]) for i in range(count)]
    for copy in own:
        copy.start()
    pl.semaphore_wait(barrier, n - 1)

    def copies(k, source):
        peer = lax.rem(me + k, n)
        return [
            pltpu.make_async_remote_copy(
                src_ref=ins[i].at[peer],
                dst_ref=outs[i].at[source],
                send_sem=send_sem.at[i, k],
                recv_sem=recv_sem.at[i, k],
                device_id=(peer // gy, lax.rem(peer, gy)),
                device_id_type=MESH,
            )
            for i in range(count)
        ]

    def send(k, c):
        for copy in copies(k, me):
            copy.start()
        return c

    lax.fori_loop(1, n, send, 0)

    def drain(k, c):
        for copy in copies(k, lax.rem(me + n - k, n)):
            copy.wait()
        return c

    lax.fori_loop(1, n, drain, 0)
    for copy in own:
        copy.wait()


def exchange(arrays, gx, gy, number):
    count = len(arrays)
    n = gx * gy
    return pl.pallas_call(
        functools.partial(exchange_kernel, gx, gy, count),
        out_shape=[jax.ShapeDtypeStruct(a.shape, a.dtype) for a in arrays],
        in_specs=[HBM] * count,
        out_specs=[HBM] * count,
        scratch_shapes=[
            pltpu.SemaphoreType.DMA((count, n)),
            pltpu.SemaphoreType.DMA((count, n)),
            pltpu.SemaphoreType.DMA((count,)),
        ],
        compiler_params=pltpu.CompilerParams(collective_id=number, has_side_effects=True),
        name=f"exchange{number}",
    )(*arrays)


def as_row(column):
    rows = column.shape[0]
    shape = (rows, LANES)
    eye = lax.broadcasted_iota(jnp.int32, shape, 0) == lax.broadcasted_iota(jnp.int32, shape, 1)
    return jnp.sum(jnp.where(eye, column, 0.0), axis=0, keepdims=True)


def as_column(row, rows, first=0):
    shape = (rows, LANES)
    eye = lax.broadcasted_iota(jnp.int32, shape, 0) + first == lax.broadcasted_iota(jnp.int32, shape, 1)
    return jnp.sum(jnp.where(eye, row, 0.0), axis=1, keepdims=True)


def coded(values):
    top = jnp.maximum(jnp.max(jnp.abs(values), axis=1, keepdims=True), 1e-30)
    code = jnp.round(values * (TOP / top)).astype(jnp.int32).astype(jnp.int16)
    return code, as_row(top * (1.0 / TOP))


def group_product(dims, grp, slot_ref, wide_ref, cols_ref, mats_of):
    cv, bps, group = dims
    dof = wide_ref.shape[-1]
    span = bps * cv
    lane = lax.broadcasted_iota(jnp.int32, (dof, LANES), 1)
    applied = []
    for tl in range(group):
        for q in range(bps):
            block = wide_ref[slot_ref[grp * group + tl, q]]
            at = (span * tl + cv * q) % LANES
            first = min(cv, LANES - at)
            cols_ref[tl, at : at + first, :] = block[:first]
            if first < cv:
                cols_ref[tl, 0 : cv - first, :] = block[first:]
    for tl in range(group):
        cols = cols_ref[tl].astype(jnp.bfloat16)
        mats = mats_of(tl).reshape(bps * dof, dof)
        prod = lax.dot_general(mats, cols, NT, preferred_element_type=jnp.float32)
        rel = (lane + (LANES * tl - span * tl) % LANES) % LANES
        one = prod[(bps - 1) * dof :]
        for q in range(bps - 2, -1, -1):
            one = jnp.where(rel < cv * (q + 1), prod[q * dof : (q + 1) * dof], one)
        applied.append(one)
    tiles = []
    for j in range(span * group // LANES):
        low, high = LANES * j // span, (LANES * (j + 1) - 1) // span
        tile = applied[high]
        for tl in range(high - 1, low - 1, -1):
            tile = jnp.where(lane < span * (tl + 1) - LANES * j, applied[tl], tile)
        tiles.append(tile)
    whole = jnp.concatenate(tiles, axis=1)
    hi = whole.astype(jnp.bfloat16)
    lo = (whole - hi.astype(jnp.float32)).astype(jnp.bfloat16)
    rows = wide_ref[pl.ds(grp * group, group)].reshape(group * cv, dof).astype(jnp.bfloat16)
    both = jnp.dot(rows, hi, preferred_element_type=jnp.float32) + jnp.dot(
        rows, lo, preferred_element_type=jnp.float32
    )
    wide_lane = lax.broadcasted_iota(jnp.int32, (cv, span * group), 1)
    out = both[(group - 1) * cv :]
    for tl in range(group - 2, -1, -1):
        out = jnp.where(wide_lane < span * (tl + 1), both[tl * cv : (tl + 1) * cv], out)
    return out


def product_kernel(dims, slot_ref, fetched_ref, stiff_ref, out_ref, wide_ref, cols_ref):
    cv, bps, group, per_step = dims
    step = pl.program_id(0)

    @pl.when(step == 0)
    def _():
        wide_ref[...] = fetched_ref[...].astype(jnp.float32)

    def body(k, c):
        out_ref[k] = group_product(
            (cv, bps, group), step * per_step + k, slot_ref, wide_ref, cols_ref,
            lambda tl: stiff_ref[k * group + tl],
        )
        return c

    lax.fori_loop(0, per_step, body, 0)


def products(fetched, stiffness, col_slot, group):
    slots, cv, dof = fetched.shape
    bps = stiffness.shape[1]
    groups = slots // group
    per_step = 4 if groups % 4 == 0 else 1
    width = group * bps * cv
    return pl.pallas_call(
        functools.partial(product_kernel, (cv, bps, group, per_step)),
        grid=(groups // per_step,),
        out_shape=jax.ShapeDtypeStruct((groups, cv, width), jnp.float32),
        in_specs=[
            SMEM,
            pl.BlockSpec((slots, cv, dof), lambda i: (0, 0, 0)),
            pl.BlockSpec((per_step * group, bps, dof, dof), lambda i: (i, 0, 0, 0)),
        ],
        out_specs=pl.BlockSpec((per_step, cv, width), lambda i: (i, 0, 0)),
        scratch_shapes=[
            pltpu.VMEM((slots, cv, dof), jnp.float32),
            pltpu.VMEM((group, LANES, dof), jnp.float32),
        ],
        compiler_params=pltpu.CompilerParams(vmem_limit_bytes=48 << 20),
        name="products",
    )(col_slot, fetched, stiffness)


def offset_at(i, side, sign, gx, gy):
    half = gx // 2
    x, y = lax.axis_index("gx"), lax.axis_index("gy")
    row = lax.rem(lax.rem(x, half) + sign * (i // gy) + half, half)
    col = lax.rem(y + sign * lax.rem(i, gy) + gy, gy)
    return (side * half + row) * gy + col


def mixed_at(k, sign, gx, gy):
    count = gx // 2 * gy
    near = lax.rem(k, 2)
    side = lax.rem(lax.axis_index("gx") // (gx // 2) + 1 + near, 2)
    return offset_at(lax.rem(k // 2 + near, count), side, sign, gx, gy)


def slot_matrix(dims, meta_land, meta_flat, side, mine):
    n, count, bps, group, send_max = dims
    each = group + group * bps
    square = (LANES, LANES)
    sub = lax.broadcasted_iota(jnp.int32, square, 0)
    lane = lax.broadcasted_iota(jnp.int32, square, 1)
    for d in range(n):
        meta_flat[d : d + 1] = meta_land[d]
    flat = meta_flat[...].astype(jnp.float32).astype(jnp.bfloat16)
    places = []
    for kk in range(2):
        owner = meta_land[kk * count + mine]
        value = owner.astype(jnp.float32)
        same = (as_column(value, LANES) == value) & (sub < lane) & (sub >= 2 * each)
        rank = jnp.sum(jnp.where(same, 1.0, 0.0), axis=0, keepdims=True)
        at = ((lax.rem(owner, count) * 2 + kk) * send_max).astype(jnp.float32) + rank
        places.append(as_column(jnp.where(owner // count == side, at, -1.0), LANES))
    second = lax.rem(lane // group, 2)
    source = lax.broadcasted_iota(jnp.int32, (n, LANES), 0)
    taken = lax.broadcasted_iota(jnp.int32, (n, LANES), 1) // (2 * group)
    pick = jnp.where(sub == second * each + lax.rem(lane, group), 1.0, 0.0).astype(jnp.bfloat16)
    every = jnp.dot(flat, pick, preferred_element_type=jnp.float32)
    place = jnp.where(second == 0, places[0], places[1])
    pieces = []
    for half in range(2 * n * group // LANES):
        first = half * (LANES // (2 * group))
        asked = jnp.sum(jnp.where(source == taken + first, every, 0.0), axis=0, keepdims=True)
        hit = sub.astype(jnp.float32) == asked + 2.0 * each
        slot = jnp.sum(jnp.where(hit, place, 0.0), axis=0, keepdims=True)
        pieces.append(jnp.where(sub.astype(jnp.float32) == slot, 1.0, 0.0))
    return jnp.concatenate(pieces, axis=1).astype(jnp.bfloat16)


def group_tail(dims, grp, slot_ref, wide_ref, cols_ref, proj_ref):
    cv, bps, group = dims
    span = bps * cv
    lane = lax.broadcasted_iota(jnp.int32, (cv, LANES), 1)
    for tl in range(group):
        for q in range(bps):
            block = wide_ref[slot_ref[q, grp * group + tl]]
            at = (span * tl + cv * q) % LANES
            first = min(cv, LANES - at)
            cols_ref[tl, at : at + first, :] = block[:first]
            if first < cv:
                cols_ref[tl, 0 : cv - first, :] = block[first:]
    ends = []
    for tl in range(group):
        cols = cols_ref[tl].astype(jnp.bfloat16)
        prod = lax.dot_general(proj_ref[grp * group + tl], cols, NT, preferred_element_type=jnp.float32)
        both = prod[:span] + prod[span:]
        rel = (lane + (LANES * tl - span * tl) % LANES) % LANES
        one = both[(bps - 1) * cv :]
        for q in range(bps - 2, -1, -1):
            one = jnp.where(rel < cv * (q + 1), both[q * cv : (q + 1) * cv], one)
        ends.append(one)
    tiles = []
    for j in range(span * group // LANES):
        low, high = LANES * j // span, (LANES * (j + 1) - 1) // span
        tile = ends[high]
        for tl in range(high - 1, low - 1, -1):
            tile = jnp.where(lane < span * (tl + 1) - LANES * j, ends[tl], tile)
        tiles.append(tile)
    return jnp.concatenate(tiles, axis=1)


def meta_row(dims, r, asked_row, pos_rows, row):
    count, bps, group, cv = dims
    each = group + group * bps
    lane = lax.broadcasted_iota(jnp.int32, (1, LANES), 1)
    for kk in range(2):
        for tl in range(group):
            t = (kk * count + r) * group + tl
            row = jnp.where(lane == kk * each + tl, asked_row[0, t], row)
            for q in range(bps):
                row = jnp.where(lane == kk * each + group + tl * bps + q, pos_rows[q, t] * cv, row)
    return row


def fused_kernel(
    dims,
    asked_ref, pos_ref, owner_ref, slot_in, prolong_in, stiff_ref,
    out_ref,
    asked_row, pos_rows, owner_row, slot_ref, prolong_ref, meta_ref,
    meta_land, meta_flat, req_ref, stage_ref, fetched_ref, wide_ref, cols_ref, mats_ref, proj_ref,
    code_ref, factor_ref, part_ref, scale_ref, select_ref, placed_ref, total_ref,
    sent_ref, sent_scale, land_ref, land_scale, final_ref,
    meta_send, meta_recv, fetch_send, fetch_recv, part_send, part_recv, scale_send, scale_recv,
    row_send, row_recv, unit_send, unit_recv, out_sem, mats_sem, own_sem,
):
    gx, gy, cv, bps, group, send_max = dims
    n = gx * gy
    count = n // 2
    span = bps * cv
    width = group * span
    each = group + group * bps
    steps = cv // ROWS
    slots = 2 * send_max
    me = lax.axis_index("gx") * gy + lax.axis_index("gy")
    side, mine = me // count, lax.rem(me, count)
    barrier = pltpu.get_barrier_semaphore()

    def where(peer):
        return (peer // gy, lax.rem(peer, gy))

    def remote(src, dst, send_sem, recv_sem, peer):
        return pltpu.make_async_remote_copy(
            src_ref=src, dst_ref=dst, send_sem=send_sem, recv_sem=recv_sem,
            device_id=where(peer), device_id_type=MESH,
        )

    def meta_copy(peer, source):
        return remote(
            meta_ref.at[lax.rem(peer, count)], meta_land.at[source],
            meta_send.at[peer], meta_recv.at[source], peer,
        )

    def fetch_copy(peer, source):
        return remote(
            stage_ref.at[pl.ds(peer * group, group)],
            fetched_ref.at[pl.ds(source * group, group)],
            fetch_send.at[peer], fetch_recv.at[source], peer,
        )

    def part_copy(h, peer, source):
        return remote(
            code_ref.at[lax.rem(peer, count), h], part_ref.at[source, h],
            part_send.at[h, peer], part_recv.at[h, source], peer,
        )

    def scale_copy(peer, source):
        return remote(
            factor_ref.at[lax.rem(peer, count)], scale_ref.at[source],
            scale_send.at[peer], scale_recv.at[source], peer,
        )

    def row_copies(h, peer, source):
        device = side * count + peer
        return (
            remote(
                sent_scale.at[h, peer], land_scale.at[h, source],
                unit_send.at[h, peer], unit_recv.at[h, source], device,
            ),
            remote(
                sent_ref.at[h, peer], land_ref.at[h, source],
                row_send.at[h, peer], row_recv.at[h, source], device,
            ),
        )

    def out_copies(h, source):
        rows = pl.ds(h * ROWS, ROWS)
        return [
            pltpu.make_async_copy(
                final_ref.at[source, pl.ds(kk * send_max, send_max), rows],
                out_ref.at[pl.ds((kk * count + source) * send_max, send_max), rows],
                out_sem.at[h, kk * count + source],
            )
            for kk in range(2)
        ]

    def by_turn(i, sign):
        i = lax.rem(i, 2) * (count // 2) + i // 2
        return lax.rem(offset_at(i, side, sign, gx, gy), count)

    def mats_copy(peer):
        return pltpu.make_async_copy(
            stiff_ref.at[pl.ds(peer * group, group)],
            mats_ref.at[pl.ds(peer * group, group)],
            mats_sem.at[peer],
        )

    def greet(k, c):
        pl.semaphore_signal(barrier, inc=1, device_id=where(lax.rem(me + k, n)), device_id_type=MESH)
        return c

    small = [
        pltpu.make_async_copy(src, dst, own_sem.at[2 + i])
        for i, (src, dst) in enumerate((
            (asked_ref, asked_row), (pos_ref, pos_rows), (owner_ref, owner_row),
            (prolong_in, prolong_ref), (slot_in, slot_ref),
        ))
    ]
    for copy in small:
        copy.start()
    lax.fori_loop(1, n, greet, 0)
    for copy in small[:3]:
        copy.wait()
    owners = jnp.zeros((1, LANES), jnp.int32)
    for a in range(owner_row.shape[1]):
        at = lax.broadcasted_iota(jnp.int32, (1, LANES), 1) == 2 * each + a
        owners = jnp.where(at, owner_row[0, a], owners)

    def note(r, c):
        meta_ref[r] = meta_row((count, bps, group, cv), r, asked_row, pos_rows, owners)
        return c

    lax.fori_loop(0, count, note, 0, unroll=2)
    own_meta = pltpu.make_async_copy(meta_ref.at[lax.rem(me, count)], meta_land.at[me], own_sem.at[0])
    mats_copy(me).start()

    def load(k, c):
        mats_copy(mixed_at(k, -1, gx, gy)).start()
        return c

    lax.fori_loop(0, n - 1, load, 0)
    own_meta.start()
    pl.semaphore_wait(barrier, n - 1)

    def ask(k, c):
        meta_copy(mixed_at(k, 1, gx, gy), me).start()
        return c

    lax.fori_loop(0, n - 1, ask, 0)
    own_meta.wait()

    def asked(k, c):
        source = mixed_at(k, -1, gx, gy)
        meta_copy(source, source).wait()
        return c

    lax.fori_loop(0, n - 1, asked, 0)
    to_scalars = pltpu.make_async_copy(meta_land, req_ref, own_sem.at[1])
    to_scalars.start()
    small[3].wait()
    small[4].wait()
    to_scalars.wait()
    first = side * each

    def fill(k, c):
        peer = mixed_at(k, 1, gx, gy)
        for j in range(group):
            stage_ref[peer * group + j] = prolong_ref[req_ref[peer, 0, first + j]]
        return c

    lax.fori_loop(0, n - 1, fill, 0)
    for j in range(group):
        stage_ref[me * group + j] = prolong_ref[req_ref[me, 0, first + j]]

    def answer(k, c):
        fetch_copy(mixed_at(k, 1, gx, gy), me).start()
        return c

    lax.fori_loop(0, n - 1, answer, 0)

    def project(source, from_ref):
        mats_copy(source).wait()
        for j in range(group):
            t = source * group + j
            block = from_ref[t]
            wide_ref[t] = block.astype(jnp.float32)
            mats = mats_ref[t]
            mats = jnp.concatenate([mats[q] for q in range(bps)], axis=1)
            prod = jnp.dot(block, mats, preferred_element_type=jnp.float32)
            rows = jnp.concatenate([prod[:, q * LANES : (q + 1) * LANES] for q in range(bps)], axis=0)
            hi = rows.astype(jnp.bfloat16)
            proj_ref[t, 0:span] = hi
            proj_ref[t, span : 2 * span] = (rows - hi.astype(jnp.float32)).astype(jnp.bfloat16)

    select_ref[...] = slot_matrix((n, count, bps, group, send_max), meta_land, meta_flat, side, mine)
    project(me, stage_ref)

    def take(k, c):
        source = mixed_at(k, -1, gx, gy)
        fetch_copy(source, source).wait_recv()
        project(source, fetched_ref)
        return c

    lax.fori_loop(0, n - 1, take, 0)

    def send(h, j, both):
        i = lax.rem(j + 1, count)
        far = offset_at(i, 1 - side, 1, gx, gy)
        near = offset_at(i, side, 1, gx, gy)
        for peer in (far, near) if both else (far,):
            if h == 0:
                scale_copy(peer, me).start()
            part_copy(h, peer, me).start()

    def work(g, c):
        for v in range(DEEP):
            at = lax.rem(offset_at(lax.rem(g * DEEP + v + 1, count), side, 1, gx, gy), count)
            for u in range(2):
                out = group_tail(
                    (cv, bps, group), u * count + at, slot_ref, wide_ref, cols_ref.at[2 * v + u], proj_ref
                )
                top = jnp.maximum(jnp.max(jnp.abs(out), axis=1, keepdims=True), 1e-30)
                code = jnp.round(out * (TOP / top)).astype(jnp.int32)
                for h in range(steps):
                    code_ref[at, h, u] = code[h * ROWS : (h + 1) * ROWS].astype(jnp.int16)
                factor_ref[at, u] = as_row(top * (1.0 / TOP))

        @pl.when(g > 0)
        def _():
            for v in range(DEEP):
                send(0, (g - 1) * DEEP + v, True)

        return c

    lax.fori_loop(0, count // DEEP, work, 0)
    for v in range(DEEP):
        send(0, count - DEEP + v, v < DEEP - 1)
    part_ref[me] = code_ref[mine]
    scale_ref[me] = factor_ref[mine]
    for h in range(1, steps):

        def more(j, c):
            send(h, j, True)
            return c

        lax.fori_loop(0, count - 1, more, 0)
        send(h, count - 1, False)

    lane = lax.broadcasted_iota(jnp.int32, (ROWS, LANES), 1)
    column = [(lane + LANES * j) // cv * cv for j in range(width // LANES)]

    def place(h, d):
        for kk in range(2):
            v = part_ref[d, h, kk].astype(jnp.int32).astype(jnp.float32)
            v = v * as_column(scale_ref[d, kk], ROWS, h * ROWS)
            for tl in range(group):
                begin = span * tl
                low, high = begin // LANES * LANES, (begin + span - 1) // LANES * LANES
                x = v[:, low : low + LANES]
                if high > low:
                    x = jnp.where(lane >= begin % LANES, x, v[:, high : high + LANES])
                tiles = [jnp.zeros((ROWS, LANES), jnp.float32) for _ in column]
                for q in range(bps):
                    pos = req_ref[d, 0, kk * each + group + tl * bps + q]
                    moved = pltpu.roll(x, (pos + (-begin - cv * q) % LANES) & (LANES - 1), 1)
                    tiles = [jnp.where(col == pos, moved, tile) for col, tile in zip(column, tiles)]
                p = (d * 2 + kk) * group + tl
                for j, tile in enumerate(tiles):
                    placed_ref[j, pl.ds(pl.multiple_of(p * ROWS, ROWS), ROWS), :] = tile

    def decode(h, source):
        values = land_ref[h, source].astype(jnp.int32).astype(jnp.float32)
        values = values * as_column(land_scale[h, source], slots * ROWS)
        final_ref[source, :, h * ROWS : (h + 1) * ROWS, :] = values.reshape(slots, ROWS, width)

    def decode_all(h):
        def some(g, c):
            turns = [lax.rem(g * PAIR + u, count) for u in range(1, PAIR + 1)]
            sources = [by_turn(i, -1) for i in turns]
            for i, source in zip(turns, sources):

                @pl.when(i > 0)
                def _():
                    for copy in row_copies(h, source, source):
                        copy.wait_recv()

            for source in sources:
                decode(h, source)
            for source in sources:
                for copy in out_copies(h, source):
                    copy.start()
            return c

        lax.fori_loop(0, count // PAIR, some, 0)

    for h in range(steps):

        def arrive(g, c):
            turns = [lax.rem(g * PAIR + u, count) for u in range(1, PAIR + 1)]
            sources = []
            for i in turns:
                at = lax.rem(offset_at(i, side, -1, gx, gy), count)
                far, near = (1 - side) * count + at, side * count + at

                def landed(source):
                    if h == 0:
                        scale_copy(source, source).wait_recv()
                    part_copy(h, source, source).wait_recv()

                landed(far)

                @pl.when(i > 0)
                def _():
                    landed(near)

                sources += [far, near]
            for source in sources:
                place(h, source)
            return c

        lax.fori_loop(0, count // PAIR, arrive, 0)

        def gather(g, c):
            select = select_ref[...]
            for u in range(PAIR):
                rows = pl.ds(g * PAIR + u, 2 * n * group, stride=ROWS)
                x = jnp.concatenate([placed_ref[j, rows, :] for j in range(len(column))], axis=1)
                hi = x.astype(jnp.bfloat16)
                lo = (x - hi.astype(jnp.float32)).astype(jnp.bfloat16)
                got = jnp.dot(select, hi, preferred_element_type=jnp.float32)
                total_ref[g * PAIR + u] = got + jnp.dot(select, lo, preferred_element_type=jnp.float32)
            return c

        lax.fori_loop(0, ROWS // PAIR, gather, 0)

        def pack(i, own):
            peer = by_turn(i, 1)
            values = total_ref[:, pl.ds(pl.multiple_of(peer * slots, slots), slots), :]
            values = jnp.swapaxes(values, 0, 1).reshape(slots * ROWS, width)
            code, scale = coded(values)
            if own:
                land_ref[h, mine], land_scale[h, mine] = code, scale
            else:
                sent_ref[h, peer], sent_scale[h, peer] = code, scale

        def hand(i):
            for copy in row_copies(h, by_turn(i, 1), mine):
                copy.start()

        for u in range(1, PAIR + 1):
            pack(u, False)

        def pass_on(g, c):
            for u in range(1, PAIR + 1):
                pack(g * PAIR + u, False)
            for u in range(1, PAIR + 1):
                hand(g * PAIR - PAIR + u)
            return c

        lax.fori_loop(1, count // PAIR - 1, pass_on, 0)
        for u in range(count - PAIR + 1, count + 1):
            pack(u % count, u == count)
        for u in range(count - 2 * PAIR + 1, count):
            hand(u)
        if h > 0:
            decode_all(h - 1)
    decode_all(steps - 1)

    def drain(k, c):
        peer = mixed_at(k, 1, gx, gy)
        fetch_copy(peer, me).wait_send()
        scale_copy(peer, me).wait_send()
        for h in range(steps):
            part_copy(h, peer, me).wait_send()
        return c

    lax.fori_loop(0, n - 1, drain, 0)

    def finish(i, c):
        for h in range(steps):
            for copy in row_copies(h, by_turn(i, 1), mine):
                copy.wait_send()
        return c

    lax.fori_loop(1, count, finish, 0)

    def written(i, c):
        for h in range(steps):
            for copy in out_copies(h, i):
                copy.wait()
        return c

    lax.fori_loop(0, count, written, 0)


def fused(asked, pos, owners, slots_of, prolong, stiffness, gx, gy, group, send_max):
    slots, bps, dof, _ = stiffness.shape
    cv = prolong.shape[1]
    n = gx * gy
    count = n // 2
    width = group * bps * cv
    steps = cv // ROWS
    taken = 2 * n * group
    rows = 2 * send_max * ROWS
    sem = pltpu.SemaphoreType.DMA
    return pl.pallas_call(
        functools.partial(fused_kernel, (gx, gy, cv, bps, group, send_max)),
        out_shape=jax.ShapeDtypeStruct((n * send_max, cv, width), jnp.float32),
        in_specs=[HBM] * 6,
        out_specs=HBM,
        scratch_shapes=[
            pltpu.SMEM(asked.shape, jnp.int32),
            pltpu.SMEM(pos.shape, jnp.int32),
            pltpu.SMEM(owners.shape, jnp.int32),
            pltpu.SMEM(slots_of.shape, jnp.int32),
            pltpu.VMEM(prolong.shape, jnp.bfloat16),
            pltpu.VMEM((count, 1, LANES), jnp.int32),
            pltpu.VMEM((n, 1, LANES), jnp.int32),
            pltpu.VMEM((n, LANES), jnp.int32),
            pltpu.SMEM((n, 1, LANES), jnp.int32),
            pltpu.VMEM((slots, cv, dof), jnp.bfloat16),
            pltpu.VMEM((slots, cv, dof), jnp.bfloat16),
            pltpu.VMEM((slots, cv, dof), jnp.float32),
            pltpu.VMEM((2 * DEEP, group, LANES, dof), jnp.float32),
            pltpu.VMEM((slots, bps, dof, dof), jnp.bfloat16),
            pltpu.VMEM((slots, 2 * bps * cv, dof), jnp.bfloat16),
            pltpu.VMEM((count, steps, 2, ROWS, width), jnp.int16),
            pltpu.VMEM((count, 2, 1, LANES), jnp.float32),
            pltpu.VMEM((n, steps, 2, ROWS, width), jnp.int16),
            pltpu.VMEM((n, 2, 1, LANES), jnp.float32),
            pltpu.VMEM((n * send_max, taken), jnp.bfloat16),
            pltpu.VMEM((width // LANES, taken * ROWS, LANES), jnp.float32),
            pltpu.VMEM((ROWS, n * send_max, width), jnp.float32),
            pltpu.VMEM((steps, count, rows, width), jnp.int16),
            pltpu.VMEM((steps, count, 1, LANES), jnp.float32),
            pltpu.VMEM((steps, count, rows, width), jnp.int16),
            pltpu.VMEM((steps, count, 1, LANES), jnp.float32),
            pltpu.VMEM((count, 2 * send_max, cv, width), jnp.float32),
        ]
        + [sem((n,))] * 4
        + [sem((steps, n))] * 2
        + [sem((n,))] * 2
        + [sem((steps, count))] * 4
        + [sem((steps, n)), sem((n,)), sem((7,))],
        compiler_params=pltpu.CompilerParams(
            collective_id=1, has_side_effects=True, vmem_limit_bytes=47 << 20
        ),
        name="fused",
    )(asked, pos, owners, slots_of, prolong, stiffness)


def gather_rows_kernel(dims, meta_ref, owner_ref, part_ref, *refs):
    cv, bps, per_peer, group, send_max = dims
    out_ref, out_scale_ref, total_ref, place_ref, seen_ref = refs
    n = out_ref.shape[0]
    groups, _, width = part_ref.shape
    span = width // group
    total_ref[...] = jnp.zeros_like(total_ref)

    def clear(i, c):
        seen_ref[i] = 0
        return c

    lax.fori_loop(0, n, clear, 0)

    def rank(a, c):
        owner = owner_ref[a]
        before = seen_ref[owner]
        place_ref[a] = owner * send_max + before
        seen_ref[owner] = before + 1
        return c

    lax.fori_loop(0, owner_ref.shape[0], rank, 0)
    lane = lax.broadcasted_iota(jnp.int32, (cv, width), 1)
    column = lax.broadcasted_iota(jnp.int32, (width, width), 0)
    row_lane = lax.broadcasted_iota(jnp.int32, (1, width), 1)

    def body(g, c):
        at = row_lane
        for j in range(group * bps):
            t = g * group + j // bps
            pos = meta_ref[t // per_peer, 0, per_peer + (t % per_peer) * bps + j % bps]
            at = at + jnp.where(row_lane // cv == j, cv * (pos - j), 0)
        hot = jnp.where(column == at, 1.0, 0.0).astype(jnp.bfloat16)
        rest = part_ref[g]
        pieces = []
        for _ in range(3):
            piece = rest.astype(jnp.bfloat16).astype(jnp.float32)
            pieces.append(piece)
            rest = rest - piece
        placed = 0.0
        for piece in pieces:
            stack = jnp.concatenate(
                [
                    jnp.where((lane >= span * tl) & (lane < span * (tl + 1)), piece, 0.0)
                    for tl in range(group)
                ],
                axis=0,
            ).astype(jnp.bfloat16)
            placed = placed + lax.dot_general(
                stack, hot, NT, preferred_element_type=jnp.float32
            )
        for tl in range(group):
            t = g * group + tl
            where = place_ref[meta_ref[t // per_peer, 0, t % per_peer]]
            rows = placed[tl * cv : (tl + 1) * cv]
            total_ref[where] = total_ref[where] + rows
        return c

    lax.fori_loop(0, groups, body, 0, unroll=4)

    def emit(p, c):
        rows = total_ref[pl.ds(p * send_max, send_max)].reshape(send_max * cv, width)
        out_ref[p], out_scale_ref[p] = coded(rows)
        return c

    lax.fori_loop(0, n, emit, 0, unroll=4)


def gathered_rows(part, meta, owners, n, send_max, group, bps, per_peer):
    groups, cv, width = part.shape
    return pl.pallas_call(
        functools.partial(gather_rows_kernel, (cv, bps, per_peer, group, send_max)),
        out_shape=[
            jax.ShapeDtypeStruct((n, send_max * cv, width), jnp.int16),
            jax.ShapeDtypeStruct((n, 1, LANES), jnp.float32),
        ],
        in_specs=[SMEM, SMEM, VMEM],
        out_specs=[VMEM, VMEM],
        scratch_shapes=[
            pltpu.VMEM((n * send_max, cv, width), jnp.float32),
            pltpu.SMEM((owners.shape[0],), jnp.int32),
            pltpu.SMEM((n,), jnp.int32),
        ],
        compiler_params=pltpu.CompilerParams(vmem_limit_bytes=48 << 20),
        name="gathered_rows",
    )(meta, owners, part)


def per_device(gx, gy, prolong, stiffness, request, col_slot, col_pos, coarse_owner):
    n = gx * gy
    own_aggs, cv, dof = prolong.shape
    slots, bps = col_slot.shape
    per_peer = slots // n
    group = MAXNB // bps
    send_max = (2 * own_aggs + n - 1) // n
    each = per_peer + per_peer * bps
    halved = per_peer == group and gx % 2 == 0 and slots == LANES and cv % ROWS == 0 and 2 * group == ROWS == 2 * send_max and 2 * each + own_aggs <= LANES

    if halved:
        held = (request[None], col_pos.T, coarse_owner.T, col_slot.T, prolong, stiffness)
        held = [pltpu.with_memory_space_constraint(a, pltpu.HBM) for a in held]
        return fused(*held, gx, gy, group, send_max)
    meta = jnp.concatenate([request.reshape(n, per_peer), col_pos.reshape(n, per_peer * bps)], axis=1)
    meta = jnp.pad(meta, ((0, 0), (0, LANES - each)))[:, None, :]
    (meta_in,) = exchange([meta], gx, gy, 1)
    answer = prolong[meta_in[:, 0, :per_peer].reshape(-1)].reshape(n, per_peer * cv, dof)
    (fetched,) = exchange([answer], gx, gy, 2)
    made = products(fetched.reshape(slots, cv, dof), stiffness, col_slot, group)
    flat = made.reshape(slots // group, cv, group, bps * cv).transpose(0, 2, 1, 3)
    (flat,) = exchange([flat.reshape(n, per_peer * cv, bps * cv)], gx, gy, 3)
    flat = flat.reshape(slots // group, group, cv, bps * cv).transpose(0, 2, 1, 3)
    part = flat.reshape(slots // group, cv, group * bps * cv)
    code, factor = gathered_rows(part, meta_in, coarse_owner[:, 0], n, send_max, group, bps, per_peer)
    return delivered(code, factor, cv, gx, gy)


def solution(mesh):
    gx, gy = mesh.shape["gx"], mesh.shape["gy"]
    placed = (
        P(AXES, None, None),
        P(AXES, None, None, None),
        P(AXES),
        P(AXES, None),
        P(AXES, None),
        P(AXES, None),
    )
    return jax.shard_map(
        functools.partial(per_device, gx, gy),
        mesh=mesh,
        in_specs=placed,
        out_specs=P(AXES, None, None),
        check_vma=False,
    )
```

```python
import functools

import jax
import jax.numpy as jnp
from jax import lax
from jax.experimental import pallas as pl
from jax.experimental.pallas import tpu as pltpu
from jax.sharding import PartitionSpec as P

MAXNB = 16
AXES = ("gx", "gy")
LANES = 128
TOP = 32767.0
ROWS = 8
PAIR = 1
DEEP = 1
MESH = pl.DeviceIdType.MESH
HBM = pl.BlockSpec(memory_space=pl.ANY)
VMEM = pl.BlockSpec(memory_space=pltpu.VMEM)
SMEM = pl.BlockSpec(memory_space=pltpu.SMEM)
NT = (((1,), (1,)), ((), ()))


def peer_at(k, gx, gy, mixed):
    n = gx * gy
    x, y = lax.axis_index("gx"), lax.axis_index("gy")
    if gx % 2:
        return lax.rem(x * gy + y + 1 + k, n)
    half = gx // 2
    count = half * gy
    if mixed:
        near, i = lax.rem(k, 2), k // 2
    else:
        near, i = k // count, lax.rem(k, count)
    i = lax.rem(i + near, count)
    side = lax.rem(x // half + 1 + near, 2)
    row = side * half + lax.rem(x + i // gy, half)
    return row * gy + lax.rem(y + i, gy)


def deliver_kernel(dims, code_ref, scale_ref, out_ref, land_ref, land_scale, wide_ref, *sems):
    gx, gy, cv = dims
    code_send, code_recv, scale_send, scale_recv, out_sem = sems
    n, rows, width = code_ref.shape
    take = rows // cv
    me = lax.axis_index("gx") * gy + lax.axis_index("gy")
    barrier = pltpu.get_barrier_semaphore()

    def where(peer):
        return (peer // gy, lax.rem(peer, gy))

    def greet(k, c):
        peer = peer_at(k, gx, gy, True)
        pl.semaphore_signal(barrier, inc=1, device_id=where(peer), device_id_type=MESH)
        return c

    lax.fori_loop(0, n - 1, greet, 0)

    def copies(peer, source):
        return [
            pltpu.make_async_remote_copy(
                src_ref=src.at[peer], dst_ref=dst.at[source],
                send_sem=send.at[peer], recv_sem=recv.at[source],
                device_id=where(peer), device_id_type=MESH,
            )
            for src, dst, send, recv in (
                (scale_ref, land_scale, scale_send, scale_recv),
                (code_ref, land_ref, code_send, code_recv),
            )
        ]

    def out_copy(p):
        at = pl.ds(p * take, take)
        return pltpu.make_async_copy(wide_ref.at[at], out_ref.at[at], out_sem.at[p])

    pl.semaphore_wait(barrier, n - 1)

    def send(k, c):
        for copy in copies(peer_at(k, gx, gy, True), me):
            copy.start()
        return c

    lax.fori_loop(0, n - 1, send, 0)

    def decode(code, scale, p):
        values = code.astype(jnp.int32).astype(jnp.float32) * as_column(scale, rows)
        wide_ref[pl.ds(p * take, take)] = values.reshape(take, cv, width)
        out_copy(p).start()

    decode(code_ref[me], scale_ref[me], me)

    def drain(k, c):
        source = peer_at(k, gx, gy, True)
        for copy in copies(source, source):
            copy.wait()
        decode(land_ref[source], land_scale[source], source)
        return c

    lax.fori_loop(0, n - 1, drain, 0)

    def finish(p, c):
        out_copy(p).wait()
        return c

    lax.fori_loop(0, n, finish, 0)


def delivered(code, scale, cv, gx, gy):
    n, rows, width = code.shape
    sem = pltpu.SemaphoreType.DMA
    out = (n * rows // cv, cv, width)
    return pl.pallas_call(
        functools.partial(deliver_kernel, (gx, gy, cv)),
        out_shape=jax.ShapeDtypeStruct(out, jnp.float32),
        in_specs=[VMEM, VMEM],
        out_specs=HBM,
        scratch_shapes=[
            pltpu.VMEM(code.shape, jnp.int16),
            pltpu.VMEM(scale.shape, jnp.float32),
            pltpu.VMEM(out, jnp.float32),
        ]
        + [sem((n,))] * 5,
        compiler_params=pltpu.CompilerParams(
            collective_id=4, has_side_effects=True, vmem_limit_bytes=40 << 20
        ),
        name="delivered",
    )(code, scale)


def exchange_kernel(gx, gy, count, *refs):
    ins, outs = refs[:count], refs[count : 2 * count]
    send_sem, recv_sem, local_sem = refs[2 * count :]
    n = gx * gy
    me = lax.axis_index("gx") * gy + lax.axis_index("gy")
    barrier = pltpu.get_barrier_semaphore()

    def greet(k, c):
        peer = lax.rem(me + k, n)
        pl.semaphore_signal(barrier, inc=1, device_id=(peer // gy, lax.rem(peer, gy)), device_id_type=MESH)
        return c

    lax.fori_loop(1, n, greet, 0)
    own = [pltpu.make_async_copy(ins[i].at[me], outs[i].at[me], local_sem.at[i]) for i in range(count)]
    for copy in own:
        copy.start()
    pl.semaphore_wait(barrier, n - 1)

    def copies(k, source):
        peer = lax.rem(me + k, n)
        return [
            pltpu.make_async_remote_copy(
                src_ref=ins[i].at[peer],
                dst_ref=outs[i].at[source],
                send_sem=send_sem.at[i, k],
                recv_sem=recv_sem.at[i, k],
                device_id=(peer // gy, lax.rem(peer, gy)),
                device_id_type=MESH,
            )
            for i in range(count)
        ]

    def send(k, c):
        for copy in copies(k, me):
            copy.start()
        return c

    lax.fori_loop(1, n, send, 0)

    def drain(k, c):
        for copy in copies(k, lax.rem(me + n - k, n)):
            copy.wait()
        return c

    lax.fori_loop(1, n, drain, 0)
    for copy in own:
        copy.wait()


def exchange(arrays, gx, gy, number):
    count = len(arrays)
    n = gx * gy
    return pl.pallas_call(
        functools.partial(exchange_kernel, gx, gy, count),
        out_shape=[jax.ShapeDtypeStruct(a.shape, a.dtype) for a in arrays],
        in_specs=[HBM] * count,
        out_specs=[HBM] * count,
        scratch_shapes=[
            pltpu.SemaphoreType.DMA((count, n)),
            pltpu.SemaphoreType.DMA((count, n)),
            pltpu.SemaphoreType.DMA((count,)),
        ],
        compiler_params=pltpu.CompilerParams(collective_id=number, has_side_effects=True),
        name=f"exchange{number}",
    )(*arrays)


def as_row(column):
    rows = column.shape[0]
    shape = (rows, LANES)
    eye = lax.broadcasted_iota(jnp.int32, shape, 0) == lax.broadcasted_iota(jnp.int32, shape, 1)
    return jnp.sum(jnp.where(eye, column, 0.0), axis=0, keepdims=True)


def as_column(row, rows, first=0):
    shape = (rows, LANES)
    eye = lax.broadcasted_iota(jnp.int32, shape, 0) + first == lax.broadcasted_iota(jnp.int32, shape, 1)
    return jnp.sum(jnp.where(eye, row, 0.0), axis=1, keepdims=True)


def coded(values):
    top = jnp.maximum(jnp.max(jnp.abs(values), axis=1, keepdims=True), 1e-30)
    code = jnp.round(values * (TOP / top)).astype(jnp.int32).astype(jnp.int16)
    return code, as_row(top * (1.0 / TOP))


def group_product(dims, grp, slot_ref, wide_ref, cols_ref, mats_of):
    cv, bps, group = dims
    dof = wide_ref.shape[-1]
    span = bps * cv
    lane = lax.broadcasted_iota(jnp.int32, (dof, LANES), 1)
    applied = []
    for tl in range(group):
        for q in range(bps):
            block = wide_ref[slot_ref[grp * group + tl, q]]
            at = (span * tl + cv * q) % LANES
            first = min(cv, LANES - at)
            cols_ref[tl, at : at + first, :] = block[:first]
            if first < cv:
                cols_ref[tl, 0 : cv - first, :] = block[first:]
    for tl in range(group):
        cols = cols_ref[tl].astype(jnp.bfloat16)
        mats = mats_of(tl).reshape(bps * dof, dof)
        prod = lax.dot_general(mats, cols, NT, preferred_element_type=jnp.float32)
        rel = (lane + (LANES * tl - span * tl) % LANES) % LANES
        one = prod[(bps - 1) * dof :]
        for q in range(bps - 2, -1, -1):
            one = jnp.where(rel < cv * (q + 1), prod[q * dof : (q + 1) * dof], one)
        applied.append(one)
    tiles = []
    for j in range(span * group // LANES):
        low, high = LANES * j // span, (LANES * (j + 1) - 1) // span
        tile = applied[high]
        for tl in range(high - 1, low - 1, -1):
            tile = jnp.where(lane < span * (tl + 1) - LANES * j, applied[tl], tile)
        tiles.append(tile)
    whole = jnp.concatenate(tiles, axis=1)
    hi = whole.astype(jnp.bfloat16)
    lo = (whole - hi.astype(jnp.float32)).astype(jnp.bfloat16)
    rows = wide_ref[pl.ds(grp * group, group)].reshape(group * cv, dof).astype(jnp.bfloat16)
    both = jnp.dot(rows, hi, preferred_element_type=jnp.float32) + jnp.dot(
        rows, lo, preferred_element_type=jnp.float32
    )
    wide_lane = lax.broadcasted_iota(jnp.int32, (cv, span * group), 1)
    out = both[(group - 1) * cv :]
    for tl in range(group - 2, -1, -1):
        out = jnp.where(wide_lane < span * (tl + 1), both[tl * cv : (tl + 1) * cv], out)
    return out


def product_kernel(dims, slot_ref, fetched_ref, stiff_ref, out_ref, wide_ref, cols_ref):
    cv, bps, group, per_step = dims
    step = pl.program_id(0)

    @pl.when(step == 0)
    def _():
        wide_ref[...] = fetched_ref[...].astype(jnp.float32)

    def body(k, c):
        out_ref[k] = group_product(
            (cv, bps, group), step * per_step + k, slot_ref, wide_ref, cols_ref,
            lambda tl: stiff_ref[k * group + tl],
        )
        return c

    lax.fori_loop(0, per_step, body, 0)


def products(fetched, stiffness, col_slot, group):
    slots, cv, dof = fetched.shape
    bps = stiffness.shape[1]
    groups = slots // group
    per_step = 4 if groups % 4 == 0 else 1
    width = group * bps * cv
    return pl.pallas_call(
        functools.partial(product_kernel, (cv, bps, group, per_step)),
        grid=(groups // per_step,),
        out_shape=jax.ShapeDtypeStruct((groups, cv, width), jnp.float32),
        in_specs=[
            SMEM,
            pl.BlockSpec((slots, cv, dof), lambda i: (0, 0, 0)),
            pl.BlockSpec((per_step * group, bps, dof, dof), lambda i: (i, 0, 0, 0)),
        ],
        out_specs=pl.BlockSpec((per_step, cv, width), lambda i: (i, 0, 0)),
        scratch_shapes=[
            pltpu.VMEM((slots, cv, dof), jnp.float32),
            pltpu.VMEM((group, LANES, dof), jnp.float32),
        ],
        compiler_params=pltpu.CompilerParams(vmem_limit_bytes=48 << 20),
        name="products",
    )(col_slot, fetched, stiffness)


def offset_at(i, side, sign, gx, gy):
    half = gx // 2
    x, y = lax.axis_index("gx"), lax.axis_index("gy")
    row = lax.rem(lax.rem(x, half) + sign * (i // gy) + half, half)
    col = lax.rem(y + sign * lax.rem(i, gy) + gy, gy)
    return (side * half + row) * gy + col


def mixed_at(k, sign, gx, gy):
    count = gx // 2 * gy
    near = lax.rem(k, 2)
    side = lax.rem(lax.axis_index("gx") // (gx // 2) + 1 + near, 2)
    return offset_at(lax.rem(k // 2 + near, count), side, sign, gx, gy)


def slot_matrix(dims, meta_land, meta_flat, side, mine):
    n, count, bps, group, send_max = dims
    each = group + group * bps
    square = (LANES, LANES)
    sub = lax.broadcasted_iota(jnp.int32, square, 0)
    lane = lax.broadcasted_iota(jnp.int32, square, 1)
    for d in range(n):
        meta_flat[d : d + 1] = meta_land[d]
    flat = meta_flat[...].astype(jnp.float32).astype(jnp.bfloat16)
    places = []
    for kk in range(2):
        owner = meta_land[kk * count + mine]
        value = owner.astype(jnp.float32)
        same = (as_column(value, LANES) == value) & (sub < lane) & (sub >= 2 * each)
        rank = jnp.sum(jnp.where(same, 1.0, 0.0), axis=0, keepdims=True)
        at = ((lax.rem(owner, count) * 2 + kk) * send_max).astype(jnp.float32) + rank
        places.append(as_column(jnp.where(owner // count == side, at, -1.0), LANES))
    second = lax.rem(lane // group, 2)
    source = lax.broadcasted_iota(jnp.int32, (n, LANES), 0)
    taken = lax.broadcasted_iota(jnp.int32, (n, LANES), 1) // (2 * group)
    pick = jnp.where(sub == second * each + lax.rem(lane, group), 1.0, 0.0).astype(jnp.bfloat16)
    every = jnp.dot(flat, pick, preferred_element_type=jnp.float32)
    place = jnp.where(second == 0, places[0], places[1])
    pieces = []
    for half in range(2 * n * group // LANES):
        first = half * (LANES // (2 * group))
        asked = jnp.sum(jnp.where(source == taken + first, every, 0.0), axis=0, keepdims=True)
        hit = sub.astype(jnp.float32) == asked + 2.0 * each
        slot = jnp.sum(jnp.where(hit, place, 0.0), axis=0, keepdims=True)
        pieces.append(jnp.where(sub.astype(jnp.float32) == slot, 1.0, 0.0))
    return jnp.concatenate(pieces, axis=1).astype(jnp.bfloat16)


def group_tail(dims, grp, slot_ref, wide_ref, cols_ref, proj_ref):
    cv, bps, group = dims
    span = bps * cv
    lane = lax.broadcasted_iota(jnp.int32, (cv, LANES), 1)
    for tl in range(group):
        for q in range(bps):
            block = wide_ref[slot_ref[q, grp * group + tl]]
            at = (span * tl + cv * q) % LANES
            first = min(cv, LANES - at)
            cols_ref[tl, at : at + first, :] = block[:first]
            if first < cv:
                cols_ref[tl, 0 : cv - first, :] = block[first:]
    ends = []
    for tl in range(group):
        cols = cols_ref[tl].astype(jnp.bfloat16)
        prod = lax.dot_general(proj_ref[grp * group + tl], cols, NT, preferred_element_type=jnp.float32)
        both = prod[:span] + prod[span:]
        rel = (lane + (LANES * tl - span * tl) % LANES) % LANES
        one = both[(bps - 1) * cv :]
        for q in range(bps - 2, -1, -1):
            one = jnp.where(rel < cv * (q + 1), both[q * cv : (q + 1) * cv], one)
        ends.append(one)
    tiles = []
    for j in range(span * group // LANES):
        low, high = LANES * j // span, (LANES * (j + 1) - 1) // span
        tile = ends[high]
        for tl in range(high - 1, low - 1, -1):
            tile = jnp.where(lane < span * (tl + 1) - LANES * j, ends[tl], tile)
        tiles.append(tile)
    return jnp.concatenate(tiles, axis=1)


def meta_row(dims, r, asked_row, pos_rows, row):
    count, bps, group, cv = dims
    each = group + group * bps
    lane = lax.broadcasted_iota(jnp.int32, (1, LANES), 1)
    for kk in range(2):
        for tl in range(group):
            t = (kk * count + r) * group + tl
            row = jnp.where(lane == kk * each + tl, asked_row[0, t], row)
            for q in range(bps):
                row = jnp.where(lane == kk * each + group + tl * bps + q, pos_rows[q, t] * cv, row)
    return row


def fused_kernel(
    dims,
    asked_ref, pos_ref, owner_ref, slot_in, prolong_in, stiff_ref,
    out_ref,
    asked_row, pos_rows, owner_row, slot_ref, prolong_ref, meta_ref,
    meta_land, meta_flat, req_ref, stage_ref, fetched_ref, wide_ref, cols_ref, mats_ref, proj_ref,
    code_ref, factor_ref, part_ref, scale_ref, select_ref, placed_ref, total_ref,
    sent_ref, sent_scale, land_ref, land_scale, final_ref,
    meta_send, meta_recv, fetch_send, fetch_recv, part_send, part_recv, scale_send, scale_recv,
    row_send, row_recv, unit_send, unit_recv, out_sem, mats_sem, own_sem,
):
    gx, gy, cv, bps, group, send_max = dims
    n = gx * gy
    count = n // 2
    span = bps * cv
    width = group * span
    each = group + group * bps
    steps = cv // ROWS
    slots = 2 * send_max
    me = lax.axis_index("gx") * gy + lax.axis_index("gy")
    side, mine = me // count, lax.rem(me, count)
    barrier = pltpu.get_barrier_semaphore()

    def where(peer):
        return (peer // gy, lax.rem(peer, gy))

    def remote(src, dst, send_sem, recv_sem, peer, device=None):
        return pltpu.make_async_remote_copy(
            src_ref=src, dst_ref=dst, send_sem=send_sem, recv_sem=recv_sem,
            device_id=where(peer) if device is None else device, device_id_type=MESH,
        )

    def meta_copy(peer, source):
        return remote(
            meta_ref.at[lax.rem(peer, count)], meta_land.at[source],
            meta_send.at[peer], meta_recv.at[source], peer,
        )

    def fetch_copy(peer, source):
        return remote(
            stage_ref.at[pl.ds(peer * group, group)],
            fetched_ref.at[pl.ds(source * group, group)],
            fetch_send.at[peer], fetch_recv.at[source], peer,
        )

    def part_copy(h, peer, source, at=None, device=None):
        at = lax.rem(peer, count) if at is None else at
        return remote(
            code_ref.at[at, h], part_ref.at[source, h],
            part_send.at[h, peer], part_recv.at[h, source], peer, device,
        )

    def scale_copy(peer, source, at=None, device=None):
        at = lax.rem(peer, count) if at is None else at
        return remote(
            factor_ref.at[at], scale_ref.at[source],
            scale_send.at[peer], scale_recv.at[source], peer, device,
        )

    def row_copies(h, peer, source):
        device = side * count + peer
        return (
            remote(
                sent_scale.at[h, peer], land_scale.at[h, source],
                unit_send.at[h, peer], unit_recv.at[h, source], device,
            ),
            remote(
                sent_ref.at[h, peer], land_ref.at[h, source],
                row_send.at[h, peer], row_recv.at[h, source], device,
            ),
        )

    def out_copies(h, source):
        rows = pl.ds(h * ROWS, ROWS)
        return [
            pltpu.make_async_copy(
                final_ref.at[source, pl.ds(kk * send_max, send_max), rows],
                out_ref.at[pl.ds((kk * count + source) * send_max, send_max), rows],
                out_sem.at[h, kk * count + source],
            )
            for kk in range(2)
        ]

    def by_turn(i, sign):
        i = lax.rem(i, 2) * (count // 2) + i // 2
        return lax.rem(offset_at(i, side, sign, gx, gy), count)

    def mats_copy(peer):
        return pltpu.make_async_copy(
            stiff_ref.at[pl.ds(peer * group, group)],
            mats_ref.at[pl.ds(peer * group, group)],
            mats_sem.at[peer],
        )

    def greet(k, c):
        pl.semaphore_signal(barrier, inc=1, device_id=where(lax.rem(me + k, n)), device_id_type=MESH)
        return c

    small = [
        pltpu.make_async_copy(src, dst, own_sem.at[2 + i])
        for i, (src, dst) in enumerate((
            (asked_ref, asked_row), (pos_ref, pos_rows), (owner_ref, owner_row),
            (prolong_in, prolong_ref), (slot_in, slot_ref),
        ))
    ]
    for copy in small:
        copy.start()
    lax.fori_loop(1, n, greet, 0)
    for copy in small[:3]:
        copy.wait()
    owners = jnp.zeros((1, LANES), jnp.int32)
    for a in range(owner_row.shape[1]):
        at = lax.broadcasted_iota(jnp.int32, (1, LANES), 1) == 2 * each + a
        owners = jnp.where(at, owner_row[0, a], owners)

    def note(r, c):
        meta_ref[r] = meta_row((count, bps, group, cv), r, asked_row, pos_rows, owners)
        return c

    lax.fori_loop(0, count, note, 0, unroll=2)
    own_meta = pltpu.make_async_copy(meta_ref.at[lax.rem(me, count)], meta_land.at[me], own_sem.at[0])
    mats_copy(me).start()

    def load(k, c):
        mats_copy(mixed_at(k, -1, gx, gy)).start()
        return c

    lax.fori_loop(0, n - 1, load, 0)
    own_meta.start()
    pl.semaphore_wait(barrier, n - 1)

    def ask(k, c):
        meta_copy(mixed_at(k, 1, gx, gy), me).start()
        return c

    lax.fori_loop(0, n - 1, ask, 0)
    own_meta.wait()

    def asked(k, c):
        source = mixed_at(k, -1, gx, gy)
        meta_copy(source, source).wait()
        return c

    lax.fori_loop(0, n - 1, asked, 0)
    to_scalars = pltpu.make_async_copy(meta_land, req_ref, own_sem.at[1])
    to_scalars.start()
    small[3].wait()
    small[4].wait()
    to_scalars.wait()
    first = side * each

    def fill(k, c):
        peer = mixed_at(k, 1, gx, gy)
        for j in range(group):
            stage_ref[peer * group + j] = prolong_ref[req_ref[peer, 0, first + j]]
        return c

    lax.fori_loop(0, n - 1, fill, 0)
    for j in range(group):
        stage_ref[me * group + j] = prolong_ref[req_ref[me, 0, first + j]]

    def answer(k, c):
        fetch_copy(mixed_at(k, 1, gx, gy), me).start()
        return c

    lax.fori_loop(0, n - 1, answer, 0)

    def project(source, from_ref):
        mats_copy(source).wait()
        for j in range(group):
            t = source * group + j
            block = from_ref[t]
            wide_ref[t] = block.astype(jnp.float32)
            mats = mats_ref[t]
            mats = jnp.concatenate([mats[q] for q in range(bps)], axis=1)
            prod = jnp.dot(block, mats, preferred_element_type=jnp.float32)
            rows = jnp.concatenate([prod[:, q * LANES : (q + 1) * LANES] for q in range(bps)], axis=0)
            hi = rows.astype(jnp.bfloat16)
            proj_ref[t, 0:span] = hi
            proj_ref[t, span : 2 * span] = (rows - hi.astype(jnp.float32)).astype(jnp.bfloat16)

    select_ref[...] = slot_matrix((n, count, bps, group, send_max), meta_land, meta_flat, side, mine)
    project(me, stage_ref)

    def take(k, c):
        source = mixed_at(k, -1, gx, gy)
        fetch_copy(source, source).wait_recv()
        project(source, fetched_ref)
        return c

    lax.fori_loop(0, n - 1, take, 0)

    def send(h, j, both):
        half = gx // 2
        i = lax.rem(j + 1, count)
        row = lax.rem(lax.rem(lax.axis_index("gx"), half) + i // gy, half)
        col = lax.rem(lax.axis_index("gy") + lax.rem(i, gy), gy)
        at = row * gy + col
        for there in (1 - side, side) if both else (1 - side,):
            spot = (there * count + at, at, (there * half + row, col))
            if h == 0:
                scale_copy(spot[0], me, *spot[1:]).start()
            part_copy(h, spot[0], me, *spot[1:]).start()

    def work(g, c):
        for v in range(DEEP):
            at = lax.rem(offset_at(lax.rem(g * DEEP + v + 1, count), side, 1, gx, gy), count)
            for u in range(2):
                out = group_tail(
                    (cv, bps, group), u * count + at, slot_ref, wide_ref, cols_ref.at[2 * v + u], proj_ref
                )
                top = jnp.maximum(jnp.max(jnp.abs(out), axis=1, keepdims=True), 1e-30)
                code = jnp.round(out * (TOP / top)).astype(jnp.int32)
                for h in range(steps):
                    code_ref[at, h, u] = code[h * ROWS : (h + 1) * ROWS].astype(jnp.int16)
                factor_ref[at, u] = as_row(top * (1.0 / TOP))

        @pl.when(g > 0)
        def _():
            for v in range(DEEP):
                send(0, (g - 1) * DEEP + v, True)

        return c

    lax.fori_loop(0, count // DEEP, work, 0)
    for v in range(DEEP):
        send(0, count - DEEP + v, v < DEEP - 1)
    part_ref[me] = code_ref[mine]
    scale_ref[me] = factor_ref[mine]
    for h in range(1, steps):

        def more(j, c):
            send(h, j, True)
            return c

        lax.fori_loop(0, count - 1, more, 0)
        send(h, count - 1, False)

    lane = lax.broadcasted_iota(jnp.int32, (ROWS, LANES), 1)
    column = [(lane + LANES * j) // cv * cv for j in range(width // LANES)]

    def place(h, d):
        for kk in range(2):
            v = part_ref[d, h, kk].astype(jnp.int32).astype(jnp.float32)
            v = v * as_column(scale_ref[d, kk], ROWS, h * ROWS)
            for tl in range(group):
                begin = span * tl
                low, high = begin // LANES * LANES, (begin + span - 1) // LANES * LANES
                x = v[:, low : low + LANES]
                if high > low:
                    x = jnp.where(lane >= begin % LANES, x, v[:, high : high + LANES])
                tiles = [jnp.zeros((ROWS, LANES), jnp.float32) for _ in column]
                for q in range(bps):
                    pos = req_ref[d, 0, kk * each + group + tl * bps + q]
                    moved = pltpu.roll(x, (pos + (-begin - cv * q) % LANES) & (LANES - 1), 1)
                    tiles = [jnp.where(col == pos, moved, tile) for col, tile in zip(column, tiles)]
                p = (d * 2 + kk) * group + tl
                for j, tile in enumerate(tiles):
                    placed_ref[j, pl.ds(pl.multiple_of(p * ROWS, ROWS), ROWS), :] = tile

    def decode(h, source):
        values = land_ref[h, source].astype(jnp.int32).astype(jnp.float32)
        values = values * as_column(land_scale[h, source], slots * ROWS)
        final_ref[source, :, h * ROWS : (h + 1) * ROWS, :] = values.reshape(slots, ROWS, width)

    def decode_all(h):
        def some(g, c):
            turns = [lax.rem(g * PAIR + u, count) for u in range(1, PAIR + 1)]
            sources = [by_turn(i, -1) for i in turns]
            for i, source in zip(turns, sources):

                @pl.when(i > 0)
                def _():
                    for copy in row_copies(h, source, source):
                        copy.wait_recv()

            for source in sources:
                decode(h, source)
            for source in sources:
                for copy in out_copies(h, source):
                    copy.start()
            return c

        lax.fori_loop(0, count // PAIR, some, 0)

    for h in range(steps):

        def arrive(g, c):
            turns = [lax.rem(g * PAIR + u, count) for u in range(1, PAIR + 1)]
            sources = []
            for i in turns:
                at = lax.rem(offset_at(i, side, -1, gx, gy), count)
                far, near = (1 - side) * count + at, side * count + at

                def landed(source):
                    if h == 0:
                        scale_copy(source, source).wait_recv()
                    part_copy(h, source, source).wait_recv()

                landed(far)

                @pl.when(i > 0)
                def _():
                    landed(near)

                sources += [far, near]
            for source in sources:
                place(h, source)
            return c

        lax.fori_loop(0, count // PAIR, arrive, 0)

        def gather(g, c):
            select = select_ref[...]
            for u in range(PAIR):
                rows = pl.ds(g * PAIR + u, 2 * n * group, stride=ROWS)
                x = jnp.concatenate([placed_ref[j, rows, :] for j in range(len(column))], axis=1)
                hi = x.astype(jnp.bfloat16)
                lo = (x - hi.astype(jnp.float32)).astype(jnp.bfloat16)
                got = jnp.dot(select, hi, preferred_element_type=jnp.float32)
                total_ref[g * PAIR + u] = got + jnp.dot(select, lo, preferred_element_type=jnp.float32)
            return c

        lax.fori_loop(0, ROWS // PAIR, gather, 0)

        def pack(i, own):
            peer = by_turn(i, 1)
            values = total_ref[:, pl.ds(pl.multiple_of(peer * slots, slots), slots), :]
            values = jnp.swapaxes(values, 0, 1).reshape(slots * ROWS, width)
            code, scale = coded(values)
            if own:
                land_ref[h, mine], land_scale[h, mine] = code, scale
            else:
                sent_ref[h, peer], sent_scale[h, peer] = code, scale

        def hand(i):
            for copy in row_copies(h, by_turn(i, 1), mine):
                copy.start()

        for u in range(1, PAIR + 1):
            pack(u, False)

        def pass_on(g, c):
            for u in range(1, PAIR + 1):
                pack(g * PAIR + u, False)
            for u in range(1, PAIR + 1):
                hand(g * PAIR - PAIR + u)
            return c

        lax.fori_loop(1, count // PAIR - 1, pass_on, 0)
        for u in range(count - PAIR + 1, count + 1):
            pack(u % count, u == count)
        for u in range(count - 2 * PAIR + 1, count):
            hand(u)
    def drain(k, c):
        peer = mixed_at(k, 1, gx, gy)
        fetch_copy(peer, me).wait_send()
        scale_copy(peer, me).wait_send()
        for h in range(steps):
            part_copy(h, peer, me).wait_send()
        return c

    def finish(i, c, h):
        for copy in row_copies(h, by_turn(i, 1), mine):
            copy.wait_send()
        return c

    for h in range(steps):
        if h == steps - 1:
            lax.fori_loop(0, n - 1, drain, 0)
            for w in range(h):
                lax.fori_loop(1, count, functools.partial(finish, h=w), 0)
        decode_all(h)
    lax.fori_loop(1, count, functools.partial(finish, h=steps - 1), 0)

    def written(i, c):
        for h in range(steps):
            for copy in out_copies(h, i):
                copy.wait()
        return c

    lax.fori_loop(0, count, written, 0)


def fused(asked, pos, owners, slots_of, prolong, stiffness, gx, gy, group, send_max):
    slots, bps, dof, _ = stiffness.shape
    cv = prolong.shape[1]
    n = gx * gy
    count = n // 2
    width = group * bps * cv
    steps = cv // ROWS
    taken = 2 * n * group
    rows = 2 * send_max * ROWS
    sem = pltpu.SemaphoreType.DMA
    return pl.pallas_call(
        functools.partial(fused_kernel, (gx, gy, cv, bps, group, send_max)),
        out_shape=jax.ShapeDtypeStruct((n * send_max, cv, width), jnp.float32),
        in_specs=[HBM] * 6,
        out_specs=HBM,
        scratch_shapes=[
            pltpu.SMEM(asked.shape, jnp.int32),
            pltpu.SMEM(pos.shape, jnp.int32),
            pltpu.SMEM(owners.shape, jnp.int32),
            pltpu.SMEM(slots_of.shape, jnp.int32),
            pltpu.VMEM(prolong.shape, jnp.bfloat16),
            pltpu.VMEM((count, 1, LANES), jnp.int32),
            pltpu.VMEM((n, 1, LANES), jnp.int32),
            pltpu.VMEM((n, LANES), jnp.int32),
            pltpu.SMEM((n, 1, LANES), jnp.int32),
            pltpu.VMEM((slots, cv, dof), jnp.bfloat16),
            pltpu.VMEM((slots, cv, dof), jnp.bfloat16),
            pltpu.VMEM((slots, cv, dof), jnp.float32),
            pltpu.VMEM((2 * DEEP, group, LANES, dof), jnp.float32),
            pltpu.VMEM((slots, bps, dof, dof), jnp.bfloat16),
            pltpu.VMEM((slots, 2 * bps * cv, dof), jnp.bfloat16),
            pltpu.VMEM((count, steps, 2, ROWS, width), jnp.int16),
            pltpu.VMEM((count, 2, 1, LANES), jnp.float32),
            pltpu.VMEM((n, steps, 2, ROWS, width), jnp.int16),
            pltpu.VMEM((n, 2, 1, LANES), jnp.float32),
            pltpu.VMEM((n * send_max, taken), jnp.bfloat16),
            pltpu.VMEM((width // LANES, taken * ROWS, LANES), jnp.float32),
            pltpu.VMEM((ROWS, n * send_max, width), jnp.float32),
            pltpu.VMEM((steps, count, rows, width), jnp.int16),
            pltpu.VMEM((steps, count, 1, LANES), jnp.float32),
            pltpu.VMEM((steps, count, rows, width), jnp.int16),
            pltpu.VMEM((steps, count, 1, LANES), jnp.float32),
            pltpu.VMEM((count, 2 * send_max, cv, width), jnp.float32),
        ]
        + [sem((n,))] * 4
        + [sem((steps, n))] * 2
        + [sem((n,))] * 2
        + [sem((steps, count))] * 4
        + [sem((steps, n)), sem((n,)), sem((7,))],
        compiler_params=pltpu.CompilerParams(
            collective_id=1, has_side_effects=True, vmem_limit_bytes=47 << 20
        ),
        name="fused",
    )(asked, pos, owners, slots_of, prolong, stiffness)


def gather_rows_kernel(dims, meta_ref, owner_ref, part_ref, *refs):
    cv, bps, per_peer, group, send_max = dims
    out_ref, out_scale_ref, total_ref, place_ref, seen_ref = refs
    n = out_ref.shape[0]
    groups, _, width = part_ref.shape
    span = width // group
    total_ref[...] = jnp.zeros_like(total_ref)

    def clear(i, c):
        seen_ref[i] = 0
        return c

    lax.fori_loop(0, n, clear, 0)

    def rank(a, c):
        owner = owner_ref[a]
        before = seen_ref[owner]
        place_ref[a] = owner * send_max + before
        seen_ref[owner] = before + 1
        return c

    lax.fori_loop(0, owner_ref.shape[0], rank, 0)
    lane = lax.broadcasted_iota(jnp.int32, (cv, width), 1)
    column = lax.broadcasted_iota(jnp.int32, (width, width), 0)
    row_lane = lax.broadcasted_iota(jnp.int32, (1, width), 1)

    def body(g, c):
        at = row_lane
        for j in range(group * bps):
            t = g * group + j // bps
            pos = meta_ref[t // per_peer, 0, per_peer + (t % per_peer) * bps + j % bps]
            at = at + jnp.where(row_lane // cv == j, cv * (pos - j), 0)
        hot = jnp.where(column == at, 1.0, 0.0).astype(jnp.bfloat16)
        rest = part_ref[g]
        pieces = []
        for _ in range(3):
            piece = rest.astype(jnp.bfloat16).astype(jnp.float32)
            pieces.append(piece)
            rest = rest - piece
        placed = 0.0
        for piece in pieces:
            stack = jnp.concatenate(
                [
                    jnp.where((lane >= span * tl) & (lane < span * (tl + 1)), piece, 0.0)
                    for tl in range(group)
                ],
                axis=0,
            ).astype(jnp.bfloat16)
            placed = placed + lax.dot_general(
                stack, hot, NT, preferred_element_type=jnp.float32
            )
        for tl in range(group):
            t = g * group + tl
            where = place_ref[meta_ref[t // per_peer, 0, t % per_peer]]
            rows = placed[tl * cv : (tl + 1) * cv]
            total_ref[where] = total_ref[where] + rows
        return c

    lax.fori_loop(0, groups, body, 0, unroll=4)

    def emit(p, c):
        rows = total_ref[pl.ds(p * send_max, send_max)].reshape(send_max * cv, width)
        out_ref[p], out_scale_ref[p] = coded(rows)
        return c

    lax.fori_loop(0, n, emit, 0, unroll=4)


def gathered_rows(part, meta, owners, n, send_max, group, bps, per_peer):
    groups, cv, width = part.shape
    return pl.pallas_call(
        functools.partial(gather_rows_kernel, (cv, bps, per_peer, group, send_max)),
        out_shape=[
            jax.ShapeDtypeStruct((n, send_max * cv, width), jnp.int16),
            jax.ShapeDtypeStruct((n, 1, LANES), jnp.float32),
        ],
        in_specs=[SMEM, SMEM, VMEM],
        out_specs=[VMEM, VMEM],
        scratch_shapes=[
            pltpu.VMEM((n * send_max, cv, width), jnp.float32),
            pltpu.SMEM((owners.shape[0],), jnp.int32),
            pltpu.SMEM((n,), jnp.int32),
        ],
        compiler_params=pltpu.CompilerParams(vmem_limit_bytes=48 << 20),
        name="gathered_rows",
    )(meta, owners, part)


def per_device(gx, gy, prolong, stiffness, request, col_slot, col_pos, coarse_owner):
    n = gx * gy
    own_aggs, cv, dof = prolong.shape
    slots, bps = col_slot.shape
    per_peer = slots // n
    group = MAXNB // bps
    send_max = (2 * own_aggs + n - 1) // n
    each = per_peer + per_peer * bps
    halved = per_peer == group and gx % 2 == 0 and slots == LANES and cv % ROWS == 0 and 2 * group == ROWS == 2 * send_max and 2 * each + own_aggs <= LANES

    if halved:
        held = (request[None], col_pos.T, coarse_owner.T, col_slot.T, prolong, stiffness)
        held = [pltpu.with_memory_space_constraint(a, pltpu.HBM) for a in held]
        return fused(*held, gx, gy, group, send_max)
    meta = jnp.concatenate([request.reshape(n, per_peer), col_pos.reshape(n, per_peer * bps)], axis=1)
    meta = jnp.pad(meta, ((0, 0), (0, LANES - each)))[:, None, :]
    (meta_in,) = exchange([meta], gx, gy, 1)
    answer = prolong[meta_in[:, 0, :per_peer].reshape(-1)].reshape(n, per_peer * cv, dof)
    (fetched,) = exchange([answer], gx, gy, 2)
    made = products(fetched.reshape(slots, cv, dof), stiffness, col_slot, group)
    flat = made.reshape(slots // group, cv, group, bps * cv).transpose(0, 2, 1, 3)
    (flat,) = exchange([flat.reshape(n, per_peer * cv, bps * cv)], gx, gy, 3)
    flat = flat.reshape(slots // group, group, cv, bps * cv).transpose(0, 2, 1, 3)
    part = flat.reshape(slots // group, cv, group * bps * cv)
    code, factor = gathered_rows(part, meta_in, coarse_owner[:, 0], n, send_max, group, bps, per_peer)
    return delivered(code, factor, cv, gx, gy)


def solution(mesh):
    gx, gy = mesh.shape["gx"], mesh.shape["gy"]
    placed = (
        P(AXES, None, None),
        P(AXES, None, None, None),
        P(AXES),
        P(AXES, None),
        P(AXES, None),
        P(AXES, None),
    )
    return jax.shard_map(
        functools.partial(per_device, gx, gy),
        mesh=mesh,
        in_specs=placed,
        out_specs=P(AXES, None, None),
        check_vma=False,
    )
```

```python
import functools

import jax
import jax.numpy as jnp
from jax import lax
from jax.experimental import pallas as pl
from jax.experimental.pallas import tpu as pltpu
from jax.sharding import PartitionSpec as P

MAXNB = 16
AXES = ("gx", "gy")
LANES = 128
TOP = 32767.0
ROWS = 8
PAIR = 1
DEEP = 1
MESH = pl.DeviceIdType.MESH
HBM = pl.BlockSpec(memory_space=pl.ANY)
VMEM = pl.BlockSpec(memory_space=pltpu.VMEM)
SMEM = pl.BlockSpec(memory_space=pltpu.SMEM)
NT = (((1,), (1,)), ((), ()))


def peer_at(k, gx, gy, mixed):
    n = gx * gy
    x, y = lax.axis_index("gx"), lax.axis_index("gy")
    if gx % 2:
        return lax.rem(x * gy + y + 1 + k, n)
    half = gx // 2
    count = half * gy
    if mixed:
        near, i = lax.rem(k, 2), k // 2
    else:
        near, i = k // count, lax.rem(k, count)
    i = lax.rem(i + near, count)
    side = lax.rem(x // half + 1 + near, 2)
    row = side * half + lax.rem(x + i // gy, half)
    return row * gy + lax.rem(y + i, gy)


def deliver_kernel(dims, code_ref, scale_ref, out_ref, land_ref, land_scale, wide_ref, *sems):
    gx, gy, cv = dims
    code_send, code_recv, scale_send, scale_recv, out_sem = sems
    n, rows, width = code_ref.shape
    take = rows // cv
    me = lax.axis_index("gx") * gy + lax.axis_index("gy")
    barrier = pltpu.get_barrier_semaphore()

    def where(peer):
        return (peer // gy, lax.rem(peer, gy))

    def greet(k, c):
        peer = peer_at(k, gx, gy, True)
        pl.semaphore_signal(barrier, inc=1, device_id=where(peer), device_id_type=MESH)
        return c

    lax.fori_loop(0, n - 1, greet, 0)

    def copies(peer, source):
        return [
            pltpu.make_async_remote_copy(
                src_ref=src.at[peer], dst_ref=dst.at[source],
                send_sem=send.at[peer], recv_sem=recv.at[source],
                device_id=where(peer), device_id_type=MESH,
            )
            for src, dst, send, recv in (
                (scale_ref, land_scale, scale_send, scale_recv),
                (code_ref, land_ref, code_send, code_recv),
            )
        ]

    def out_copy(p):
        at = pl.ds(p * take, take)
        return pltpu.make_async_copy(wide_ref.at[at], out_ref.at[at], out_sem.at[p])

    pl.semaphore_wait(barrier, n - 1)

    def send(k, c):
        for copy in copies(peer_at(k, gx, gy, True), me):
            copy.start()
        return c

    lax.fori_loop(0, n - 1, send, 0)

    def decode(code, scale, p):
        values = code.astype(jnp.int32).astype(jnp.float32) * as_column(scale, rows)
        wide_ref[pl.ds(p * take, take)] = values.reshape(take, cv, width)
        out_copy(p).start()

    decode(code_ref[me], scale_ref[me], me)

    def drain(k, c):
        source = peer_at(k, gx, gy, True)
        for copy in copies(source, source):
            copy.wait()
        decode(land_ref[source], land_scale[source], source)
        return c

    lax.fori_loop(0, n - 1, drain, 0)

    def finish(p, c):
        out_copy(p).wait()
        return c

    lax.fori_loop(0, n, finish, 0)


def delivered(code, scale, cv, gx, gy):
    n, rows, width = code.shape
    sem = pltpu.SemaphoreType.DMA
    out = (n * rows // cv, cv, width)
    return pl.pallas_call(
        functools.partial(deliver_kernel, (gx, gy, cv)),
        out_shape=jax.ShapeDtypeStruct(out, jnp.float32),
        in_specs=[VMEM, VMEM],
        out_specs=HBM,
        scratch_shapes=[
            pltpu.VMEM(code.shape, jnp.int16),
            pltpu.VMEM(scale.shape, jnp.float32),
            pltpu.VMEM(out, jnp.float32),
        ]
        + [sem((n,))] * 5,
        compiler_params=pltpu.CompilerParams(
            collective_id=4, has_side_effects=True, vmem_limit_bytes=40 << 20
        ),
        name="delivered",
    )(code, scale)


def exchange_kernel(gx, gy, count, *refs):
    ins, outs = refs[:count], refs[count : 2 * count]
    send_sem, recv_sem, local_sem = refs[2 * count :]
    n = gx * gy
    me = lax.axis_index("gx") * gy + lax.axis_index("gy")
    barrier = pltpu.get_barrier_semaphore()

    def greet(k, c):
        peer = lax.rem(me + k, n)
        pl.semaphore_signal(barrier, inc=1, device_id=(peer // gy, lax.rem(peer, gy)), device_id_type=MESH)
        return c

    lax.fori_loop(1, n, greet, 0)
    own = [pltpu.make_async_copy(ins[i].at[me], outs[i].at[me], local_sem.at[i]) for i in range(count)]
    for copy in own:
        copy.start()
    pl.semaphore_wait(barrier, n - 1)

    def copies(k, source):
        peer = lax.rem(me + k, n)
        return [
            pltpu.make_async_remote_copy(
                src_ref=ins[i].at[peer],
                dst_ref=outs[i].at[source],
                send_sem=send_sem.at[i, k],
                recv_sem=recv_sem.at[i, k],
                device_id=(peer // gy, lax.rem(peer, gy)),
                device_id_type=MESH,
            )
            for i in range(count)
        ]

    def send(k, c):
        for copy in copies(k, me):
            copy.start()
        return c

    lax.fori_loop(1, n, send, 0)

    def drain(k, c):
        for copy in copies(k, lax.rem(me + n - k, n)):
            copy.wait()
        return c

    lax.fori_loop(1, n, drain, 0)
    for copy in own:
        copy.wait()


def exchange(arrays, gx, gy, number):
    count = len(arrays)
    n = gx * gy
    return pl.pallas_call(
        functools.partial(exchange_kernel, gx, gy, count),
        out_shape=[jax.ShapeDtypeStruct(a.shape, a.dtype) for a in arrays],
        in_specs=[HBM] * count,
        out_specs=[HBM] * count,
        scratch_shapes=[
            pltpu.SemaphoreType.DMA((count, n)),
            pltpu.SemaphoreType.DMA((count, n)),
            pltpu.SemaphoreType.DMA((count,)),
        ],
        compiler_params=pltpu.CompilerParams(collective_id=number, has_side_effects=True),
        name=f"exchange{number}",
    )(*arrays)


def as_row(column):
    rows = column.shape[0]
    shape = (rows, LANES)
    eye = lax.broadcasted_iota(jnp.int32, shape, 0) == lax.broadcasted_iota(jnp.int32, shape, 1)
    return jnp.sum(jnp.where(eye, column, 0.0), axis=0, keepdims=True)


def as_column(row, rows, first=0):
    shape = (rows, LANES)
    eye = lax.broadcasted_iota(jnp.int32, shape, 0) + first == lax.broadcasted_iota(jnp.int32, shape, 1)
    return jnp.sum(jnp.where(eye, row, 0.0), axis=1, keepdims=True)


def coded(values):
    top = jnp.maximum(jnp.max(jnp.abs(values), axis=1, keepdims=True), 1e-30)
    code = jnp.round(values * (TOP / top)).astype(jnp.int32).astype(jnp.int16)
    return code, as_row(top * (1.0 / TOP))


def group_product(dims, grp, slot_ref, wide_ref, cols_ref, mats_of):
    cv, bps, group = dims
    dof = wide_ref.shape[-1]
    span = bps * cv
    lane = lax.broadcasted_iota(jnp.int32, (dof, LANES), 1)
    applied = []
    for tl in range(group):
        for q in range(bps):
            block = wide_ref[slot_ref[grp * group + tl, q]]
            at = (span * tl + cv * q) % LANES
            first = min(cv, LANES - at)
            cols_ref[tl, at : at + first, :] = block[:first]
            if first < cv:
                cols_ref[tl, 0 : cv - first, :] = block[first:]
    for tl in range(group):
        cols = cols_ref[tl].astype(jnp.bfloat16)
        mats = mats_of(tl).reshape(bps * dof, dof)
        prod = lax.dot_general(mats, cols, NT, preferred_element_type=jnp.float32)
        rel = (lane + (LANES * tl - span * tl) % LANES) % LANES
        one = prod[(bps - 1) * dof :]
        for q in range(bps - 2, -1, -1):
            one = jnp.where(rel < cv * (q + 1), prod[q * dof : (q + 1) * dof], one)
        applied.append(one)
    tiles = []
    for j in range(span * group // LANES):
        low, high = LANES * j // span, (LANES * (j + 1) - 1) // span
        tile = applied[high]
        for tl in range(high - 1, low - 1, -1):
            tile = jnp.where(lane < span * (tl + 1) - LANES * j, applied[tl], tile)
        tiles.append(tile)
    whole = jnp.concatenate(tiles, axis=1)
    hi = whole.astype(jnp.bfloat16)
    lo = (whole - hi.astype(jnp.float32)).astype(jnp.bfloat16)
    rows = wide_ref[pl.ds(grp * group, group)].reshape(group * cv, dof).astype(jnp.bfloat16)
    both = jnp.dot(rows, hi, preferred_element_type=jnp.float32) + jnp.dot(
        rows, lo, preferred_element_type=jnp.float32
    )
    wide_lane = lax.broadcasted_iota(jnp.int32, (cv, span * group), 1)
    out = both[(group - 1) * cv :]
    for tl in range(group - 2, -1, -1):
        out = jnp.where(wide_lane < span * (tl + 1), both[tl * cv : (tl + 1) * cv], out)
    return out


def product_kernel(dims, slot_ref, fetched_ref, stiff_ref, out_ref, wide_ref, cols_ref):
    cv, bps, group, per_step = dims
    step = pl.program_id(0)

    @pl.when(step == 0)
    def _():
        wide_ref[...] = fetched_ref[...].astype(jnp.float32)

    def body(k, c):
        out_ref[k] = group_product(
            (cv, bps, group), step * per_step + k, slot_ref, wide_ref, cols_ref,
            lambda tl: stiff_ref[k * group + tl],
        )
        return c

    lax.fori_loop(0, per_step, body, 0)


def products(fetched, stiffness, col_slot, group):
    slots, cv, dof = fetched.shape
    bps = stiffness.shape[1]
    groups = slots // group
    per_step = 4 if groups % 4 == 0 else 1
    width = group * bps * cv
    return pl.pallas_call(
        functools.partial(product_kernel, (cv, bps, group, per_step)),
        grid=(groups // per_step,),
        out_shape=jax.ShapeDtypeStruct((groups, cv, width), jnp.float32),
        in_specs=[
            SMEM,
            pl.BlockSpec((slots, cv, dof), lambda i: (0, 0, 0)),
            pl.BlockSpec((per_step * group, bps, dof, dof), lambda i: (i, 0, 0, 0)),
        ],
        out_specs=pl.BlockSpec((per_step, cv, width), lambda i: (i, 0, 0)),
        scratch_shapes=[
            pltpu.VMEM((slots, cv, dof), jnp.float32),
            pltpu.VMEM((group, LANES, dof), jnp.float32),
        ],
        compiler_params=pltpu.CompilerParams(vmem_limit_bytes=48 << 20),
        name="products",
    )(col_slot, fetched, stiffness)


def offset_at(i, side, sign, gx, gy):
    half = gx // 2
    x, y = lax.axis_index("gx"), lax.axis_index("gy")
    row = lax.rem(lax.rem(x, half) + sign * (i // gy) + half, half)
    col = lax.rem(y + sign * lax.rem(i, gy) + gy, gy)
    return (side * half + row) * gy + col


def mixed_at(k, sign, gx, gy):
    count = gx // 2 * gy
    near = lax.rem(k, 2)
    side = lax.rem(lax.axis_index("gx") // (gx // 2) + 1 + near, 2)
    return offset_at(lax.rem(k // 2 + near, count), side, sign, gx, gy)


def slot_matrix(dims, meta_land, meta_flat, side, mine):
    n, count, bps, group, send_max = dims
    each = group + group * bps
    square = (LANES, LANES)
    sub = lax.broadcasted_iota(jnp.int32, square, 0)
    lane = lax.broadcasted_iota(jnp.int32, square, 1)
    for d in range(n):
        meta_flat[d : d + 1] = meta_land[d]
    flat = meta_flat[...].astype(jnp.float32).astype(jnp.bfloat16)
    places = []
    for kk in range(2):
        owner = meta_land[kk * count + mine]
        value = owner.astype(jnp.float32)
        same = (as_column(value, LANES) == value) & (sub < lane) & (sub >= 2 * each)
        rank = jnp.sum(jnp.where(same, 1.0, 0.0), axis=0, keepdims=True)
        at = ((lax.rem(owner, count) * 2 + kk) * send_max).astype(jnp.float32) + rank
        places.append(as_column(jnp.where(owner // count == side, at, -1.0), LANES))
    second = lax.rem(lane // group, 2)
    source = lax.broadcasted_iota(jnp.int32, (n, LANES), 0)
    taken = lax.broadcasted_iota(jnp.int32, (n, LANES), 1) // (2 * group)
    pick = jnp.where(sub == second * each + lax.rem(lane, group), 1.0, 0.0).astype(jnp.bfloat16)
    every = jnp.dot(flat, pick, preferred_element_type=jnp.float32)
    place = jnp.where(second == 0, places[0], places[1])
    pieces = []
    for half in range(2 * n * group // LANES):
        first = half * (LANES // (2 * group))
        asked = jnp.sum(jnp.where(source == taken + first, every, 0.0), axis=0, keepdims=True)
        hit = sub.astype(jnp.float32) == asked + 2.0 * each
        slot = jnp.sum(jnp.where(hit, place, 0.0), axis=0, keepdims=True)
        pieces.append(jnp.where(sub.astype(jnp.float32) == slot, 1.0, 0.0))
    return jnp.concatenate(pieces, axis=1).astype(jnp.bfloat16)


def group_tail(dims, grp, slot_ref, wide_ref, cols_ref, proj_ref):
    cv, bps, group = dims
    span = bps * cv
    lane = lax.broadcasted_iota(jnp.int32, (cv, LANES), 1)
    for tl in range(group):
        for q in range(bps):
            block = wide_ref[slot_ref[q, grp * group + tl]]
            at = (span * tl + cv * q) % LANES
            first = min(cv, LANES - at)
            cols_ref[tl, at : at + first, :] = block[:first]
            if first < cv:
                cols_ref[tl, 0 : cv - first, :] = block[first:]
    ends = []
    for tl in range(group):
        cols = cols_ref[tl].astype(jnp.bfloat16)
        prod = lax.dot_general(proj_ref[grp * group + tl], cols, NT, preferred_element_type=jnp.float32)
        both = prod[:span] + prod[span:]
        rel = (lane + (LANES * tl - span * tl) % LANES) % LANES
        one = both[(bps - 1) * cv :]
        for q in range(bps - 2, -1, -1):
            one = jnp.where(rel < cv * (q + 1), both[q * cv : (q + 1) * cv], one)
        ends.append(one)
    tiles = []
    for j in range(span * group // LANES):
        low, high = LANES * j // span, (LANES * (j + 1) - 1) // span
        tile = ends[high]
        for tl in range(high - 1, low - 1, -1):
            tile = jnp.where(lane < span * (tl + 1) - LANES * j, ends[tl], tile)
        tiles.append(tile)
    return jnp.concatenate(tiles, axis=1)


def meta_row(dims, r, asked_row, pos_rows, row):
    count, bps, group, cv = dims
    each = group + group * bps
    lane = lax.broadcasted_iota(jnp.int32, (1, LANES), 1)
    for kk in range(2):
        for tl in range(group):
            t = (kk * count + r) * group + tl
            row = jnp.where(lane == kk * each + tl, asked_row[0, t], row)
            for q in range(bps):
                row = jnp.where(lane == kk * each + group + tl * bps + q, pos_rows[q, t] * cv, row)
    return row


def fused_kernel(
    dims,
    asked_ref, pos_ref, owner_ref, slot_in, prolong_in, stiff_ref,
    out_ref,
    asked_row, pos_rows, owner_row, slot_ref, prolong_ref, meta_ref,
    meta_land, meta_flat, req_ref, stage_ref, fetched_ref, wide_ref, cols_ref, mats_ref, proj_ref,
    code_ref, factor_ref, part_ref, scale_ref, select_ref, placed_ref, total_ref,
    sent_ref, sent_scale, land_ref, land_scale, final_ref,
    meta_send, meta_recv, fetch_send, fetch_recv, part_send, part_recv, scale_send, scale_recv,
    row_send, row_recv, unit_send, unit_recv, out_sem, mats_sem, own_sem,
):
    gx, gy, cv, bps, group, send_max = dims
    n = gx * gy
    count = n // 2
    span = bps * cv
    width = group * span
    each = group + group * bps
    steps = cv // ROWS
    slots = 2 * send_max
    me = lax.axis_index("gx") * gy + lax.axis_index("gy")
    side, mine = me // count, lax.rem(me, count)
    barrier = pltpu.get_barrier_semaphore()

    def where(peer):
        return (peer // gy, lax.rem(peer, gy))

    def remote(src, dst, send_sem, recv_sem, peer, device=None):
        return pltpu.make_async_remote_copy(
            src_ref=src, dst_ref=dst, send_sem=send_sem, recv_sem=recv_sem,
            device_id=where(peer) if device is None else device, device_id_type=MESH,
        )

    def meta_copy(peer, source):
        return remote(
            meta_ref.at[lax.rem(peer, count)], meta_land.at[source],
            meta_send.at[peer], meta_recv.at[source], peer,
        )

    def fetch_copy(peer, source):
        return remote(
            stage_ref.at[pl.ds(peer * group, group)],
            fetched_ref.at[pl.ds(source * group, group)],
            fetch_send.at[peer], fetch_recv.at[source], peer,
        )

    def part_copy(h, peer, source, at=None, device=None):
        at = lax.rem(peer, count) if at is None else at
        return remote(
            code_ref.at[at, h], part_ref.at[source, h],
            part_send.at[h, peer], part_recv.at[h, source], peer, device,
        )

    def scale_copy(peer, source, at=None, device=None):
        at = lax.rem(peer, count) if at is None else at
        return remote(
            factor_ref.at[at], scale_ref.at[source],
            scale_send.at[peer], scale_recv.at[source], peer, device,
        )

    def row_copies(h, peer, source):
        device = side * count + peer
        return (
            remote(
                sent_scale.at[h, peer], land_scale.at[h, source],
                unit_send.at[h, peer], unit_recv.at[h, source], device,
            ),
            remote(
                sent_ref.at[h, peer], land_ref.at[h, source],
                row_send.at[h, peer], row_recv.at[h, source], device,
            ),
        )

    def out_copies(h, source):
        rows = pl.ds(h * ROWS, ROWS)
        return [
            pltpu.make_async_copy(
                final_ref.at[source, pl.ds(kk * send_max, send_max), rows],
                out_ref.at[pl.ds((kk * count + source) * send_max, send_max), rows],
                out_sem.at[h, kk * count + source],
            )
            for kk in range(2)
        ]

    def by_turn(i, sign):
        i = lax.rem(i, 2) * (count // 2) + i // 2
        return lax.rem(offset_at(i, side, sign, gx, gy), count)

    def mats_copy(peer):
        return pltpu.make_async_copy(
            stiff_ref.at[pl.ds(peer * group, group)],
            mats_ref.at[pl.ds(peer * group, group)],
            mats_sem.at[peer],
        )

    def greet(k, c):
        pl.semaphore_signal(barrier, inc=1, device_id=where(lax.rem(me + k, n)), device_id_type=MESH)
        return c

    small = [
        pltpu.make_async_copy(src, dst, own_sem.at[2 + i])
        for i, (src, dst) in enumerate((
            (asked_ref, asked_row), (pos_ref, pos_rows), (owner_ref, owner_row),
            (prolong_in, prolong_ref), (slot_in, slot_ref),
        ))
    ]
    for copy in small:
        copy.start()
    lax.fori_loop(1, n, greet, 0)
    for copy in small[:3]:
        copy.wait()
    owners = jnp.zeros((1, LANES), jnp.int32)
    for a in range(owner_row.shape[1]):
        at = lax.broadcasted_iota(jnp.int32, (1, LANES), 1) == 2 * each + a
        owners = jnp.where(at, owner_row[0, a], owners)

    def note(r, c):
        meta_ref[r] = meta_row((count, bps, group, cv), r, asked_row, pos_rows, owners)
        return c

    lax.fori_loop(0, count, note, 0, unroll=2)
    own_meta = pltpu.make_async_copy(meta_ref.at[lax.rem(me, count)], meta_land.at[me], own_sem.at[0])
    mats_copy(me).start()

    def load(k, c):
        mats_copy(mixed_at(k, -1, gx, gy)).start()
        return c

    lax.fori_loop(0, n - 1, load, 0)
    own_meta.start()
    pl.semaphore_wait(barrier, n - 1)

    def ask(k, c):
        meta_copy(mixed_at(k, 1, gx, gy), me).start()
        return c

    lax.fori_loop(0, n - 1, ask, 0)
    own_meta.wait()

    def asked(k, c):
        source = mixed_at(k, -1, gx, gy)
        meta_copy(source, source).wait()
        return c

    lax.fori_loop(0, n - 1, asked, 0)
    to_scalars = pltpu.make_async_copy(meta_land, req_ref, own_sem.at[1])
    to_scalars.start()
    small[3].wait()
    small[4].wait()
    to_scalars.wait()
    first = side * each

    def fill(k, c):
        peer = mixed_at(k, 1, gx, gy)
        for j in range(group):
            stage_ref[peer * group + j] = prolong_ref[req_ref[peer, 0, first + j]]

        @pl.when(k > 0)
        def _():
            fetch_copy(mixed_at(k - 1, 1, gx, gy), me).start()

        return c

    lax.fori_loop(0, n - 1, fill, 0)
    fetch_copy(mixed_at(n - 2, 1, gx, gy), me).start()
    for j in range(group):
        stage_ref[me * group + j] = prolong_ref[req_ref[me, 0, first + j]]


    def project(source, from_ref):
        mats_copy(source).wait()
        for j in range(group):
            t = source * group + j
            block = from_ref[t]
            wide_ref[t] = block.astype(jnp.float32)
            mats = mats_ref[t]
            mats = jnp.concatenate([mats[q] for q in range(bps)], axis=1)
            prod = jnp.dot(block, mats, preferred_element_type=jnp.float32)
            rows = jnp.concatenate([prod[:, q * LANES : (q + 1) * LANES] for q in range(bps)], axis=0)
            hi = rows.astype(jnp.bfloat16)
            proj_ref[t, 0:span] = hi
            proj_ref[t, span : 2 * span] = (rows - hi.astype(jnp.float32)).astype(jnp.bfloat16)

    select_ref[...] = slot_matrix((n, count, bps, group, send_max), meta_land, meta_flat, side, mine)
    project(me, stage_ref)

    def take(k, c):
        source = mixed_at(k, -1, gx, gy)
        fetch_copy(source, source).wait_recv()
        project(source, fetched_ref)
        return c

    lax.fori_loop(0, n - 1, take, 0)

    def send(h, j, both):
        half = gx // 2
        i = lax.rem(j + 1, count)
        row = lax.rem(lax.rem(lax.axis_index("gx"), half) + i // gy, half)
        col = lax.rem(lax.axis_index("gy") + lax.rem(i, gy), gy)
        at = row * gy + col
        for there in (1 - side, side) if both else (1 - side,):
            spot = (there * count + at, at, (there * half + row, col))
            if h == 0:
                scale_copy(spot[0], me, *spot[1:]).start()
            part_copy(h, spot[0], me, *spot[1:]).start()

    def work(g, c):
        for v in range(DEEP):
            at = lax.rem(offset_at(lax.rem(g * DEEP + v + 1, count), side, 1, gx, gy), count)
            for u in range(2):
                out = group_tail(
                    (cv, bps, group), u * count + at, slot_ref, wide_ref, cols_ref.at[2 * v + u], proj_ref
                )
                top = jnp.maximum(jnp.max(jnp.abs(out), axis=1, keepdims=True), 1e-30)
                code = jnp.round(out * (TOP / top)).astype(jnp.int32)
                for h in range(steps):
                    code_ref[at, h, u] = code[h * ROWS : (h + 1) * ROWS].astype(jnp.int16)
                factor_ref[at, u] = as_row(top * (1.0 / TOP))

        @pl.when(g > 0)
        def _():
            for v in range(DEEP):
                send(0, (g - 1) * DEEP + v, True)

        return c

    lax.fori_loop(0, count // DEEP, work, 0)
    for v in range(DEEP):
        send(0, count - DEEP + v, v < DEEP - 1)
    part_ref[me] = code_ref[mine]
    scale_ref[me] = factor_ref[mine]
    for h in range(1, steps):

        def more(j, c):
            send(h, j, True)
            return c

        lax.fori_loop(0, count - 1, more, 0)
        send(h, count - 1, False)

    lane = lax.broadcasted_iota(jnp.int32, (ROWS, LANES), 1)
    column = [(lane + LANES * j) // cv * cv for j in range(width // LANES)]

    def place(h, d):
        for kk in range(2):
            v = part_ref[d, h, kk].astype(jnp.int32).astype(jnp.float32)
            v = v * as_column(scale_ref[d, kk], ROWS, h * ROWS)
            for tl in range(group):
                begin = span * tl
                low, high = begin // LANES * LANES, (begin + span - 1) // LANES * LANES
                x = v[:, low : low + LANES]
                if high > low:
                    x = jnp.where(lane >= begin % LANES, x, v[:, high : high + LANES])
                tiles = [jnp.zeros((ROWS, LANES), jnp.float32) for _ in column]
                for q in range(bps):
                    pos = req_ref[d, 0, kk * each + group + tl * bps + q]
                    moved = pltpu.roll(x, (pos + (-begin - cv * q) % LANES) & (LANES - 1), 1)
                    tiles = [jnp.where(col == pos, moved, tile) for col, tile in zip(column, tiles)]
                p = (d * 2 + kk) * group + tl
                for j, tile in enumerate(tiles):
                    placed_ref[j, pl.ds(pl.multiple_of(p * ROWS, ROWS), ROWS), :] = tile

    def decode(h, source):
        values = land_ref[h, source].astype(jnp.int32).astype(jnp.float32)
        values = values * as_column(land_scale[h, source], slots * ROWS)
        final_ref[source, :, h * ROWS : (h + 1) * ROWS, :] = values.reshape(slots, ROWS, width)

    def decode_all(h):
        def some(g, c):
            turns = [lax.rem(g * PAIR + u, count) for u in range(1, PAIR + 1)]
            sources = [by_turn(i, -1) for i in turns]
            for i, source in zip(turns, sources):

                @pl.when(i > 0)
                def _():
                    for copy in row_copies(h, source, source):
                        copy.wait_recv()

            for source in sources:
                decode(h, source)
            for source in sources:
                for copy in out_copies(h, source):
                    copy.start()
            return c

        lax.fori_loop(0, count // PAIR, some, 0)

    for h in range(steps):

        def arrive(g, c):
            turns = [lax.rem(g * PAIR + u, count) for u in range(1, PAIR + 1)]
            sources = []
            for i in turns:
                at = lax.rem(offset_at(i, side, -1, gx, gy), count)
                far, near = (1 - side) * count + at, side * count + at

                def landed(source):
                    if h == 0:
                        scale_copy(source, source).wait_recv()
                    part_copy(h, source, source).wait_recv()

                landed(far)

                @pl.when(i > 0)
                def _():
                    landed(near)

                sources += [far, near]
            for source in sources:
                place(h, source)
            return c

        lax.fori_loop(0, count // PAIR, arrive, 0)

        def gather(g, c):
            select = select_ref[...]
            for u in range(PAIR):
                rows = pl.ds(g * PAIR + u, 2 * n * group, stride=ROWS)
                x = jnp.concatenate([placed_ref[j, rows, :] for j in range(len(column))], axis=1)
                hi = x.astype(jnp.bfloat16)
                lo = (x - hi.astype(jnp.float32)).astype(jnp.bfloat16)
                got = jnp.dot(select, hi, preferred_element_type=jnp.float32)
                total_ref[g * PAIR + u] = got + jnp.dot(select, lo, preferred_element_type=jnp.float32)
            return c

        lax.fori_loop(0, ROWS // PAIR, gather, 0)

        def pack(i, own):
            peer = by_turn(i, 1)
            values = total_ref[:, pl.ds(pl.multiple_of(peer * slots, slots), slots), :]
            values = jnp.swapaxes(values, 0, 1).reshape(slots * ROWS, width)
            code, scale = coded(values)
            if own:
                land_ref[h, mine], land_scale[h, mine] = code, scale
            else:
                sent_ref[h, peer], sent_scale[h, peer] = code, scale

        def hand(i):
            for copy in row_copies(h, by_turn(i, 1), mine):
                copy.start()

        for u in range(1, PAIR + 1):
            pack(u, False)

        def pass_on(g, c):
            for u in range(1, PAIR + 1):
                pack(g * PAIR + u, False)
            for u in range(1, PAIR + 1):
                hand(g * PAIR - PAIR + u)
            return c

        lax.fori_loop(1, count // PAIR - 1, pass_on, 0)
        for u in range(count - PAIR + 1, count + 1):
            pack(u % count, u == count)
        for u in range(count - 2 * PAIR + 1, count):
            hand(u)
    def drain(k, c):
        peer = mixed_at(k, 1, gx, gy)
        fetch_copy(peer, me).wait_send()
        scale_copy(peer, me).wait_send()
        for h in range(steps):
            part_copy(h, peer, me).wait_send()
        return c

    def finish(i, c, h):
        for copy in row_copies(h, by_turn(i, 1), mine):
            copy.wait_send()
        return c

    for h in range(steps):
        if h == steps - 1:
            lax.fori_loop(0, n - 1, drain, 0)
            for w in range(h):
                lax.fori_loop(1, count, functools.partial(finish, h=w), 0)
        decode_all(h)
    lax.fori_loop(1, count, functools.partial(finish, h=steps - 1), 0)

    def written(i, c):
        for h in range(steps):
            for copy in out_copies(h, i):
                copy.wait()
        return c

    lax.fori_loop(0, count, written, 0)


def fused(asked, pos, owners, slots_of, prolong, stiffness, gx, gy, group, send_max):
    slots, bps, dof, _ = stiffness.shape
    cv = prolong.shape[1]
    n = gx * gy
    count = n // 2
    width = group * bps * cv
    steps = cv // ROWS
    taken = 2 * n * group
    rows = 2 * send_max * ROWS
    sem = pltpu.SemaphoreType.DMA
    return pl.pallas_call(
        functools.partial(fused_kernel, (gx, gy, cv, bps, group, send_max)),
        out_shape=jax.ShapeDtypeStruct((n * send_max, cv, width), jnp.float32),
        in_specs=[HBM] * 6,
        out_specs=HBM,
        scratch_shapes=[
            pltpu.SMEM(asked.shape, jnp.int32),
            pltpu.SMEM(pos.shape, jnp.int32),
            pltpu.SMEM(owners.shape, jnp.int32),
            pltpu.SMEM(slots_of.shape, jnp.int32),
            pltpu.VMEM(prolong.shape, jnp.bfloat16),
            pltpu.VMEM((count, 1, LANES), jnp.int32),
            pltpu.VMEM((n, 1, LANES), jnp.int32),
            pltpu.VMEM((n, LANES), jnp.int32),
            pltpu.SMEM((n, 1, LANES), jnp.int32),
            pltpu.VMEM((slots, cv, dof), jnp.bfloat16),
            pltpu.VMEM((slots, cv, dof), jnp.bfloat16),
            pltpu.VMEM((slots, cv, dof), jnp.float32),
            pltpu.VMEM((2 * DEEP, group, LANES, dof), jnp.float32),
            pltpu.VMEM((slots, bps, dof, dof), jnp.bfloat16),
            pltpu.VMEM((slots, 2 * bps * cv, dof), jnp.bfloat16),
            pltpu.VMEM((count, steps, 2, ROWS, width), jnp.int16),
            pltpu.VMEM((count, 2, 1, LANES), jnp.float32),
            pltpu.VMEM((n, steps, 2, ROWS, width), jnp.int16),
            pltpu.VMEM((n, 2, 1, LANES), jnp.float32),
            pltpu.VMEM((n * send_max, taken), jnp.bfloat16),
            pltpu.VMEM((width // LANES, taken * ROWS, LANES), jnp.float32),
            pltpu.VMEM((ROWS, n * send_max, width), jnp.float32),
            pltpu.VMEM((steps, count, rows, width), jnp.int16),
            pltpu.VMEM((steps, count, 1, LANES), jnp.float32),
            pltpu.VMEM((steps, count, rows, width), jnp.int16),
            pltpu.VMEM((steps, count, 1, LANES), jnp.float32),
            pltpu.VMEM((count, 2 * send_max, cv, width), jnp.float32),
        ]
        + [sem((n,))] * 4
        + [sem((steps, n))] * 2
        + [sem((n,))] * 2
        + [sem((steps, count))] * 4
        + [sem((steps, n)), sem((n,)), sem((7,))],
        compiler_params=pltpu.CompilerParams(
            collective_id=1, has_side_effects=True, vmem_limit_bytes=47 << 20
        ),
        name="fused",
    )(asked, pos, owners, slots_of, prolong, stiffness)


def gather_rows_kernel(dims, meta_ref, owner_ref, part_ref, *refs):
    cv, bps, per_peer, group, send_max = dims
    out_ref, out_scale_ref, total_ref, place_ref, seen_ref = refs
    n = out_ref.shape[0]
    groups, _, width = part_ref.shape
    span = width // group
    total_ref[...] = jnp.zeros_like(total_ref)

    def clear(i, c):
        seen_ref[i] = 0
        return c

    lax.fori_loop(0, n, clear, 0)

    def rank(a, c):
        owner = owner_ref[a]
        before = seen_ref[owner]
        place_ref[a] = owner * send_max + before
        seen_ref[owner] = before + 1
        return c

    lax.fori_loop(0, owner_ref.shape[0], rank, 0)
    lane = lax.broadcasted_iota(jnp.int32, (cv, width), 1)
    column = lax.broadcasted_iota(jnp.int32, (width, width), 0)
    row_lane = lax.broadcasted_iota(jnp.int32, (1, width), 1)

    def body(g, c):
        at = row_lane
        for j in range(group * bps):
            t = g * group + j // bps
            pos = meta_ref[t // per_peer, 0, per_peer + (t % per_peer) * bps + j % bps]
            at = at + jnp.where(row_lane // cv == j, cv * (pos - j), 0)
        hot = jnp.where(column == at, 1.0, 0.0).astype(jnp.bfloat16)
        rest = part_ref[g]
        pieces = []
        for _ in range(3):
            piece = rest.astype(jnp.bfloat16).astype(jnp.float32)
            pieces.append(piece)
            rest = rest - piece
        placed = 0.0
        for piece in pieces:
            stack = jnp.concatenate(
                [
                    jnp.where((lane >= span * tl) & (lane < span * (tl + 1)), piece, 0.0)
                    for tl in range(group)
                ],
                axis=0,
            ).astype(jnp.bfloat16)
            placed = placed + lax.dot_general(
                stack, hot, NT, preferred_element_type=jnp.float32
            )
        for tl in range(group):
            t = g * group + tl
            where = place_ref[meta_ref[t // per_peer, 0, t % per_peer]]
            rows = placed[tl * cv : (tl + 1) * cv]
            total_ref[where] = total_ref[where] + rows
        return c

    lax.fori_loop(0, groups, body, 0, unroll=4)

    def emit(p, c):
        rows = total_ref[pl.ds(p * send_max, send_max)].reshape(send_max * cv, width)
        out_ref[p], out_scale_ref[p] = coded(rows)
        return c

    lax.fori_loop(0, n, emit, 0, unroll=4)


def gathered_rows(part, meta, owners, n, send_max, group, bps, per_peer):
    groups, cv, width = part.shape
    return pl.pallas_call(
        functools.partial(gather_rows_kernel, (cv, bps, per_peer, group, send_max)),
        out_shape=[
            jax.ShapeDtypeStruct((n, send_max * cv, width), jnp.int16),
            jax.ShapeDtypeStruct((n, 1, LANES), jnp.float32),
        ],
        in_specs=[SMEM, SMEM, VMEM],
        out_specs=[VMEM, VMEM],
        scratch_shapes=[
            pltpu.VMEM((n * send_max, cv, width), jnp.float32),
            pltpu.SMEM((owners.shape[0],), jnp.int32),
            pltpu.SMEM((n,), jnp.int32),
        ],
        compiler_params=pltpu.CompilerParams(vmem_limit_bytes=48 << 20),
        name="gathered_rows",
    )(meta, owners, part)


def per_device(gx, gy, prolong, stiffness, request, col_slot, col_pos, coarse_owner):
    n = gx * gy
    own_aggs, cv, dof = prolong.shape
    slots, bps = col_slot.shape
    per_peer = slots // n
    group = MAXNB // bps
    send_max = (2 * own_aggs + n - 1) // n
    each = per_peer + per_peer * bps
    halved = per_peer == group and gx % 2 == 0 and slots == LANES and cv % ROWS == 0 and 2 * group == ROWS == 2 * send_max and 2 * each + own_aggs <= LANES

    if halved:
        held = (request[None], col_pos.T, coarse_owner.T, col_slot.T, prolong, stiffness)
        held = [pltpu.with_memory_space_constraint(a, pltpu.HBM) for a in held]
        return fused(*held, gx, gy, group, send_max)
    meta = jnp.concatenate([request.reshape(n, per_peer), col_pos.reshape(n, per_peer * bps)], axis=1)
    meta = jnp.pad(meta, ((0, 0), (0, LANES - each)))[:, None, :]
    (meta_in,) = exchange([meta], gx, gy, 1)
    answer = prolong[meta_in[:, 0, :per_peer].reshape(-1)].reshape(n, per_peer * cv, dof)
    (fetched,) = exchange([answer], gx, gy, 2)
    made = products(fetched.reshape(slots, cv, dof), stiffness, col_slot, group)
    flat = made.reshape(slots // group, cv, group, bps * cv).transpose(0, 2, 1, 3)
    (flat,) = exchange([flat.reshape(n, per_peer * cv, bps * cv)], gx, gy, 3)
    flat = flat.reshape(slots // group, group, cv, bps * cv).transpose(0, 2, 1, 3)
    part = flat.reshape(slots // group, cv, group * bps * cv)
    code, factor = gathered_rows(part, meta_in, coarse_owner[:, 0], n, send_max, group, bps, per_peer)
    return delivered(code, factor, cv, gx, gy)


def solution(mesh):
    gx, gy = mesh.shape["gx"], mesh.shape["gy"]
    placed = (
        P(AXES, None, None),
        P(AXES, None, None, None),
        P(AXES),
        P(AXES, None),
        P(AXES, None),
        P(AXES, None),
    )
    return jax.shard_map(
        functools.partial(per_device, gx, gy),
        mesh=mesh,
        in_specs=placed,
        out_specs=P(AXES, None, None),
        check_vma=False,
    )
```
